128 devices in a mesh: batch: 4 (over y), expert: 8 (over x, core), tensor: 4 (over z).
Axes of the slice: x: 4, y: 4, z: 4, core: 2. Of those that a mesh axis runs over, the one named last changes fastest.
Arguments:
- tokens: bfloat16 [8, 1024, 4096], P('expert', 'batch', 'tensor'), may hold values from -8 to 8
- gain: bfloat16 [4096], P('tensor'), may hold values from 0.5 to 1.5
- phi: bfloat16 [4096, 512], P('tensor'), may hold values from -1 to 1
- w_gate: bfloat16 [8, 4096, 14336], P('expert', None, ('batch', 'tensor')), may hold values from -0.125 to 0.125
- w_up: bfloat16 [8, 4096, 14336], P('expert', None, ('batch', 'tensor')), may hold values from -0.125 to 0.125
- w_down: bfloat16 [8, 14336, 4096], P('expert', ('batch', 'tensor')), may hold values from -0.09375 to 0.09375
Outputs:
- moe_out: bfloat16 [8, 1024, 4096], P('expert', 'batch', 'tensor')
The draws below stay inside these ranges and needn't reach their ends.
All inputs are finite; a program needn't handle non-finite values.
Results may differ from the reference program's by a relative error of at most 0.025.
Values may be sent and summed in bfloat16 or wider, within the bound.
A program may use at most 128 MiB of HBM per device.

```python
import math
import jax
import jax.numpy as jnp
from jax import lax

D = 4096
FF = 14336
P_SIZE = 64
E = 8
GROUPS = 8
GROUP_TOK = 1024
SHARDS = 16


def draw_tokens(key, part):
    base_key = jax.random.fold_in(key, 21)
    values = jax.random.normal(base_key, (GROUPS, GROUP_TOK, D), jnp.float32)
    return jnp.clip(values, -8.0, 8.0).astype(jnp.bfloat16)


def draw_phi(key, part):
    base_draw = jax.random.normal(jax.random.fold_in(key, 31), (D, E * P_SIZE), jnp.float32) * (3.0 / math.sqrt(D))
    base_draw = jnp.clip(base_draw, -1.0, 1.0)
    return base_draw.astype(jnp.bfloat16)


def spiked(values, rng, source, target, parts, factor):
    owner, partner = [(jnp.arange(values.shape[position]) // (values.shape[position] // parts)).reshape([-1 if axis == position else 1 for axis in range(values.ndim)]) for position in (source, target)]
    chosen = jax.random.permutation(rng, parts)[partner]
    strong = (owner == chosen) | (owner == (partner + parts // 2) % parts)
    return jnp.where(strong, factor * values, values)


def steps_of(own_key, dims, cuts, least, top_value):
    factor_of = 1.0
    for position, blocks in cuts:
        heights = jax.random.uniform(jax.random.fold_in(jax.random.fold_in(own_key, 6), position), (blocks,), jnp.float32, least / len(cuts), top_value / len(cuts))
        factor_of = factor_of * jnp.repeat(jnp.exp(heights), dims[position] // blocks).reshape((-1,) + (1,) * (len(dims) - 1 - position))
    return factor_of


def noise(key, shape, deviation, most, split=(), kind=jnp.bfloat16):
    drawn = deviation * jax.random.normal(key, shape, jnp.float32)
    if split:
        drawn = drawn * steps_of(key, shape, split, -0.22, 0.18)
    return jnp.clip(drawn, -most, most).astype(kind)


def gaussian_with(own_key, shape, width, bound, shards, heavy, kind=jnp.bfloat16):
    values = width * jax.random.normal(own_key, shape, jnp.float32)
    if shards:
        values = values * steps_of(own_key, shape, shards, -0.22, 0.18)
    return jnp.clip(spiked(values, jax.random.fold_in(own_key, 3), *heavy), -bound, bound).astype(kind)


def setup_inputs(seed: int = 0) -> dict:
    splits = jax.random.split(jax.random.key(seed), 7)
    return {
        "tokens": draw_tokens(jax.random.fold_in(splits[6], 71), 0),
        "gain": jnp.clip(1.0 + 0.1 * jax.random.normal(splits[1], (D,), jnp.float32), 0.5, 1.5).astype(jnp.bfloat16),
        "phi": draw_phi(jax.random.fold_in(splits[6], 71), 0),
        "w_gate": noise(splits[3], (E, D, FF), (D // 2) ** -0.5, 0.125, ((0, 8), (2, 16))),
        "w_up": noise(splits[4], (E, D, FF), (D // 2) ** -0.5, 0.125, ((0, 8), (2, 16))),
        "w_down": gaussian_with(splits[5], (E, FF, D), (FF // 2) ** -0.5, 0.09375, ((0, 8), (1, 16)), (1, 2, 16, 2.0)),
    }


def reference(tokens, gain, phi, w_gate, w_up, w_down):
    tokens_f = tokens.astype(jnp.float32)
    gain_f = gain.astype(jnp.float32)
    scaled = (tokens_f * gain_f).astype(jnp.bfloat16)
    inv_rms = lax.rsqrt(lax.optimization_barrier(jnp.mean(tokens_f * tokens_f, axis=2)) + 1e-06)
    logits = jnp.einsum('gnd,ds->gns', scaled.astype(jnp.float32), phi.astype(jnp.float32)) * inv_rms[:, :, None]
    normed = (tokens_f * gain_f * inv_rms[:, :, None]).astype(jnp.bfloat16)
    column_max = lax.optimization_barrier(jnp.max(logits, axis=1, keepdims=True))
    raised = jnp.exp(logits - column_max)
    dispatch = (raised / lax.optimization_barrier(jnp.sum(raised, axis=1, keepdims=True))).astype(jnp.bfloat16)
    combine = jax.nn.softmax(logits, axis=2).astype(jnp.bfloat16)
    slot_in = jnp.einsum('gns,gnd->gsd', dispatch.astype(jnp.float32), normed.astype(jnp.float32)).astype(jnp.bfloat16)
    per_expert = slot_in.reshape(GROUPS, E, P_SIZE, D).transpose(1, 0, 2, 3).reshape(E, GROUPS * P_SIZE, D)

    def run_expert(expert_items):
        slot_rows, gate_weight, up_weight, down_weight = expert_items
        gate_act = jnp.dot(slot_rows, gate_weight, preferred_element_type=jnp.float32)
        up_act = jnp.dot(slot_rows, up_weight, preferred_element_type=jnp.float32)
        hidden = (jax.nn.silu(gate_act) * up_act).astype(jnp.bfloat16)
        block_width = FF // SHARDS
        pieces = hidden.reshape(GROUPS * P_SIZE, SHARDS, block_width).transpose(1, 0, 2).astype(jnp.float32)
        weights = down_weight.reshape(SHARDS, block_width, D).astype(jnp.float32)
        partials = jnp.einsum('krf,kfd->krd', pieces, weights).astype(jnp.bfloat16)
        partials = lax.optimization_barrier(partials)
        return lax.optimization_barrier(jnp.sum(partials.astype(jnp.float32), axis=0)).astype(jnp.bfloat16)
    slot_out = lax.map(run_expert, (per_expert, w_gate, w_up, w_down))
    slot_out = slot_out.reshape(E, GROUPS, P_SIZE, D).transpose(1, 0, 2, 3).reshape(GROUPS, E * P_SIZE, D)
    moe_out = jnp.einsum('gns,gsd->gnd', combine.astype(jnp.float32), slot_out.astype(jnp.float32))
    return moe_out.astype(jnp.bfloat16)
```

```python
import jax
import jax.numpy as jnp
from jax import lax
from jax.experimental import pallas as pl
from jax.experimental.pallas import tpu as pltpu
from jax.sharding import PartitionSpec as P


D = 4096
RING = 4
BF16 = jnp.bfloat16
F32 = jnp.float32


def near(v):
    return lax.rem(v + 2 * RING, RING)


class Net:
    def __init__(self, send_sems, recv_sems):
        self.send_sems, self.recv_sems = send_sems, recv_sems
        self.used, self.sent = 0, []

    def take(self, count=1):
        first = self.used
        self.used += count
        return first

    def copy(self, n, src, dst, target):
        return pltpu.make_async_remote_copy(
            src_ref=src,
            dst_ref=dst,
            send_sem=self.send_sems.at[n],
            recv_sem=self.recv_sems.at[n],
            device_id=target,
            device_id_type=pl.DeviceIdType.MESH,
        )

    def start(self, n, src, dst, target):
        one = self.copy(n, src, dst, target)
        one.start()
        self.sent.append(one)

    def arrived(self, n, dst, target):
        self.copy(n, dst, dst, target).wait_recv()

    def drain(self):
        for one in self.sent:
            one.wait_send()


class Gather:
    def __init__(self, net, axis, me, d, ref):
        self.net, self.axis, self.me, self.d, self.ref = net, axis, me, d, ref
        self.n = net.take(3)

    def to(self, d):
        return {self.axis: near(self.me + d)}

    def start(self):
        mine = self.ref(self.me)
        self.net.start(self.n, mine, mine, self.to(self.d))
        self.net.start(self.n + 1, mine, mine, self.to(-self.d))

    def relay(self):
        block = self.ref(near(self.me - self.d))
        self.net.arrived(self.n, block, self.to(self.d))
        self.net.start(self.n + 2, block, block, self.to(self.d))

    def direct(self):
        self.net.arrived(self.n + 1, self.ref(near(self.me + self.d)), self.to(self.d))

    def last(self):
        self.net.arrived(self.n + 2, self.ref(near(self.me + 2)), self.to(self.d))


class Scatter:
    def __init__(self, net, axis, me, d, part, buffers):
        self.net, self.axis, self.me, self.d, self.part = net, axis, me, d, part
        self.passing, self.direct_in, self.joined = buffers
        self.n = net.take(3)

    def to(self, d):
        return {self.axis: near(self.me + d)}

    def send_far(self):
        self.net.start(self.n, self.part(near(self.me + 2)), self.passing, self.to(self.d))

    def send_near(self):
        self.net.start(self.n + 1, self.part(near(self.me - self.d)), self.direct_in, self.to(-self.d))

    def relay(self):
        self.net.arrived(self.n, self.passing, self.to(self.d))
        term = self.part(near(self.me + self.d))
        total = term[...].astype(F32) + self.passing[...].astype(F32)
        term[...] = total.astype(term.dtype)
        self.net.start(self.n + 2, term, self.joined, self.to(self.d))

    def finish(self):
        self.net.arrived(self.n + 1, self.direct_in, self.to(self.d))
        self.net.arrived(self.n + 2, self.joined, self.to(self.d))
        mine = self.part(self.me)[...].astype(F32)
        return mine + self.direct_in[...].astype(F32) + self.joined[...].astype(F32)


def kernel(
    tok_in, gain, phi_in, wg_in, wu_in, wd_in, out,
    tok, phi, wg, wu, wd, sc,
    lp, l_in, sq_out, sq_in, st, qb, cb, qn,
    cs, c_in, si, xs, acc, hid, ys,
    a_in, a_sum, a2_in, b_in, b_sum, b2_in, so, rf,
    load_sems, send_sems, recv_sems,
):
    y = lax.axis_index("batch")
    e = lax.axis_index("expert")
    z = lax.axis_index("tensor")
    x, c = e // 2, lax.rem(e, 2)

    loads = [
        pltpu.make_async_copy(src, dst, load_sems.at[i])
        for i, (src, dst) in enumerate(
            ((tok_in, tok), (phi_in, phi), (wg_in, wg), (wu_in, wu), (wd_in, wd))
        )
    ]
    loads[0].start()
    loads[1].start()

    barrier = pltpu.get_barrier_semaphore()
    plane = [(dy, dz) for dy in range(RING) for dz in range(RING) if (dy, dz) != (0, 0)]
    across = [(dx, dc) for dx in (2, 1, 3, 0) for dc in range(2) if (dx, dc) != (0, 0)]

    def in_plane(dy, dz):
        return {"batch": near(y + dy), "tensor": near(z + dz)}

    def over_x(dx, dc):
        return {"expert": near(x + dx) * 2 + lax.rem(c + dc, 2)}

    peers = [in_plane(*step) for step in plane] + [over_x(*step) for step in across]
    for peer in peers:
        pl.semaphore_signal(
            barrier, inc=1, device_id=peer, device_id_type=pl.DeviceIdType.MESH
        )

    net = Net(send_sems, recv_sems)

    loads[0].wait()
    tokens_f = tok[...].astype(F32)
    sc[...] = (tokens_f * gain[...].astype(F32)).astype(BF16)
    squares = jnp.sum(tokens_f * tokens_f, axis=1, keepdims=True)
    rows = lp.shape[1]
    diagonal = lax.broadcasted_iota(jnp.int32, (rows, 128), 0) == lax.broadcasted_iota(
        jnp.int32, (rows, 128), 1
    )
    for b in range(RING):
        column = squares[b * rows : (b + 1) * rows]
        line = jnp.sum(jnp.where(diagonal, column, 0.0), axis=0, keepdims=True)
        sq_out[b] = jnp.broadcast_to(line, (8, 128))
    loads[1].wait()
    for b in range(RING):
        part = jnp.dot(
            sc[b * rows : (b + 1) * rows, :], phi[...], preferred_element_type=F32
        )
        lp[b] = part
    for one in loads[2:]:
        one.start()

    pl.semaphore_wait(barrier, len(peers))

    half = rows // 2
    logit_pieces = [
        Scatter(
            net, "tensor", z, d,
            lambda b, i=i: lp.at[b, pl.ds(i * half, half)],
            [l_in.at[k, i] for k in range(3)],
        )
        for i, d in enumerate((1, -1))
    ]
    for piece in logit_pieces:
        piece.send_far()
    first_sq = net.take(3)
    for k in range(3):
        to = near(z + k + 1)
        net.start(first_sq + k, sq_out.at[to], sq_in.at[k], {"tensor": to})
    for piece in logit_pieces:
        piece.send_near()
    for piece in logit_pieces:
        piece.relay()
    for k in range(3):
        net.arrived(first_sq + k, sq_in.at[k], {"tensor": near(z + k + 1)})
    sq = sq_out[z] + sq_in[0] + sq_in[1] + sq_in[2]
    sq_column = jnp.sum(jnp.where(diagonal, sq[0:1, :], 0.0), axis=1, keepdims=True)
    inv_rms = lax.rsqrt(sq_column / D + 1e-06)
    logits = jnp.concatenate([piece.finish() for piece in logit_pieces], axis=0) * inv_rms

    local_max = jnp.max(logits, axis=0, keepdims=True)
    raised = jnp.exp(logits - local_max)
    local_total = jnp.sum(raised, axis=0, keepdims=True)
    mine = st.at[y, z]
    for k in range(4):
        mine[k : k + 1, :] = local_max[:, k * 128 : (k + 1) * 128]
        mine[4 + k : 5 + k, :] = local_total[:, k * 128 : (k + 1) * 128]
    qb[z] = (raised * inv_rms).astype(BF16)
    first_st = net.take(len(plane))
    q_pieces = [
        Gather(net, "tensor", z, d, lambda b, i=i: qb.at[b, pl.ds(i * half, half)])
        for i, d in enumerate((1, -1))
    ]
    for piece in q_pieces:
        piece.start()
    for k, step in enumerate(plane):
        net.start(first_st + k, mine, mine, in_plane(*step))

    row_max = jnp.max(logits, axis=1, keepdims=True)
    row_raised = jnp.exp(logits - row_max)
    cb[z] = (row_raised / jnp.sum(row_raised, axis=1, keepdims=True)).astype(BF16)
    for piece in q_pieces:
        piece.relay()
    mix_pieces = [
        Gather(net, "tensor", z, d, lambda b, i=i: cb.at[b, pl.ds(i * half, half)])
        for i, d in enumerate((1, -1))
    ]
    for piece in mix_pieces:
        piece.start()
    for k, (dy, dz) in enumerate(plane):
        net.arrived(first_st + k, st.at[near(y - dy), near(z - dz)], in_plane(dy, dz))
    stats = st[...]
    maxima, totals = stats[:, :, 0:4, :], stats[:, :, 4:8, :]
    top = jnp.max(jnp.max(maxima, axis=1), axis=0)
    total = jnp.sum(jnp.sum(totals * jnp.exp(maxima - top[None, None]), axis=1), axis=0)
    factor = jnp.exp(st[y][:, 0:4, :] - top[None]) / total[None]
    for piece in q_pieces:
        piece.direct()
    for piece in q_pieces:
        piece.last()
    for b in range(RING):
        line = jnp.concatenate([factor[b, k : k + 1, :] for k in range(4)], axis=1)
        qn[b * rows : (b + 1) * rows, :] = (qb[b].astype(F32) * line).astype(BF16)
    for piece in mix_pieces:
        piece.relay()

    width = sc.shape[1]
    tile = 256

    @pl.loop(0, width // tile)
    def _(j):
        at = pl.ds(pl.multiple_of(j * tile, tile), tile)
        part = lax.dot_general(
            qn[...], sc[:, at], (((0,), (0,)), ((), ())), preferred_element_type=F32
        )
        cs[:, :, :, at] = part.astype(BF16).reshape(8, RING, 16, tile)

    pairs = [near(x + k) for k in (2, 1, 3, 0)]
    slot_pieces = [
        Scatter(
            net, "batch", y, d,
            lambda b, i=i: cs.at[pl.ds(2 * i, 2), b],
            [c_in.at[k, i] for k in range(3)],
        )
        for i, d in enumerate((1, -1, 1, -1))
    ]
    for piece in slot_pieces:
        piece.send_far()
    for piece in slot_pieces:
        piece.send_near()
    for piece in slot_pieces:
        piece.relay()
    for i, piece in enumerate(slot_pieces):
        si[2 * i : 2 * i + 2] = piece.finish().astype(BF16)

    def place(k, core):
        return xs.at[z, k // 2, y, pl.ds(lax.rem(k, 2) * 32 + core * 16, 16)]

    first_x = net.take(len(across))
    for n, (dx, dc) in enumerate(across):
        target = over_x(dx, dc)
        net.start(
            first_x + n, si.at[target["expert"]], place((RING - dx) % RING, c), target
        )
    place(0, c)[...] = si[e]

    def wait_x(k):
        for n, (dx, dc) in enumerate(across):
            if (RING - dx) % RING == k:
                net.arrived(first_x + n, place(k, lax.rem(c + dc, 2)), over_x(dx, dc))

    def strip(h, i):
        return pl.ds(i * 32, 32)

    a1 = [
        Gather(net, "batch", y, d, lambda b, i=i: xs.at[z, 0, b, pl.ds(i * 32, 32)])
        for i, d in enumerate((1, -1))
    ]
    b1 = [
        Gather(net, "tensor", z, d, lambda b, i=i: xs.at[b, 1, y, pl.ds(i * 32, 32)])
        for i, d in enumerate((1, -1))
    ]
    steps = (0, 3, 1, 2)
    ways = (1, 1, -1, -1)
    a2 = [
        Gather(net, "tensor", z, d, lambda b, j=j: xs.at[b, 0, near(y + j)])
        for j, d in zip(steps, ways)
    ]
    b2 = [
        Gather(net, "batch", y, d, lambda b, j=j: xs.at[near(z + j), 1, b])
        for j, d in zip(steps, ways)
    ]

    for k in (0, 1):
        wait_x(k)
        a1[k].start()
    for k in (2, 3):
        wait_x(k)
        b1[k - 2].start()
    a2[0].start()
    b2[0].start()
    for stage in (a1, b1):
        for piece in stage:
            piece.relay()
    for stage, later in ((a1, a2), (b1, b2)):
        for piece in stage:
            piece.direct()
        later[1].start()
        later[2].start()
    for stage, later in ((a1, a2), (b1, b2)):
        for piece in stage:
            piece.last()
        later[3].start()

    loads[2].wait()
    loads[3].wait()
    share = acc.shape[0]

    def raise_rows(h, b, first):
        deep = pl.ds(pl.multiple_of(b * width, width), width)
        block = xs[b, h].reshape(RING * 64, width)

        @pl.loop(0, share)
        def _(j):
            at = pl.ds(pl.multiple_of(j * 128, 128), 128)
            both = jnp.concatenate([wg[deep, at], wu[deep, at]], axis=1)
            part = jnp.dot(block, both, preferred_element_type=F32)
            if first:
                acc[j, h] = part
            else:
                acc[j, h] = acc[j, h] + part

    def close_rows(h):
        @pl.loop(0, share)
        def _(j):
            at = pl.ds(pl.multiple_of(j * 128, 128), 128)
            gate, up = acc[j, h][:, :128], acc[j, h][:, 128:]
            hid[h, :, at] = (gate / (1.0 + jnp.exp(-gate)) * up).astype(BF16)

    raise_rows(0, z, True)
    a2[0].relay()
    b2[0].relay()
    a2[2].relay()
    b2[2].relay()
    b2[0].direct()
    a2[1].relay()
    b2[1].relay()
    b2[0].last()
    raise_rows(1, z, True)
    a2[3].relay()
    b2[3].relay()
    for piece in a2:
        piece.direct()
    raise_rows(0, near(z - 1), False)
    raise_rows(0, near(z + 1), False)
    b2[1].direct()
    b2[1].last()
    raise_rows(1, near(z - 1), False)
    b2[2].direct()
    b2[2].last()
    raise_rows(1, near(z + 1), False)
    for piece in a2:
        piece.last()
    raise_rows(0, near(z + 2), False)
    close_rows(0)

    loads[4].wait()

    def lower_rows(h, b):
        @pl.loop(0, width // tile)
        def _(j):
            inside = pl.ds(pl.multiple_of(j * tile, tile), tile)
            at = pl.ds(pl.multiple_of(b * width + j * tile, tile), tile)
            part = jnp.dot(hid[h], wd[:, at], preferred_element_type=F32)
            ys[b, h, :, :, inside] = part.astype(BF16).reshape(RING, 64, tile)

    order = (2, 1, 3, 0)
    sides = (1, -1, 1, -1)
    ra1 = [
        Scatter(
            net, "tensor", z, d,
            lambda b, j=j: ys.at[b, 0, near(y + j)],
            [a_in.at[k, i] for k in range(3)],
        )
        for i, (j, d) in enumerate(zip(order, sides))
    ]
    rb1 = [
        Scatter(
            net, "batch", y, d,
            lambda b, j=j: ys.at[near(z + j), 1, b],
            [b_in.at[k, i] for k in range(3)],
        )
        for i, (j, d) in enumerate(zip(order, sides))
    ]
    ra2 = [
        Scatter(
            net, "batch", y, d,
            lambda b, i=i: a_sum.at[b, pl.ds(i * 32, 32)],
            [a2_in.at[k, i] for k in range(3)],
        )
        for i, d in enumerate((1, -1))
    ]
    rb2 = [
        Scatter(
            net, "tensor", z, d,
            lambda b, i=i: b_sum.at[b, pl.ds(i * 32, 32)],
            [b2_in.at[k, i] for k in range(3)],
        )
        for i, d in enumerate((1, -1))
    ]

    lower_rows(0, near(z + 2))
    for piece in ra1:
        piece.send_far()
    b2[3].direct()
    b2[3].last()
    raise_rows(1, near(z + 2), False)
    close_rows(1)
    lower_rows(1, near(z + 2))
    rb1[0].send_far()
    rb1[0].send_near()
    lower_rows(0, near(z + 1))
    ra1[1].send_near()
    ra1[3].send_near()
    lower_rows(1, near(z + 1))
    rb1[1].send_far()
    rb1[1].send_near()
    lower_rows(0, near(z - 1))
    ra1[0].send_near()
    ra1[2].send_near()
    lower_rows(1, near(z - 1))
    rb1[2].send_far()
    rb1[2].send_near()
    ra1[0].relay()
    ra1[1].relay()
    rb1[0].relay()
    lower_rows(1, z)
    rb1[3].send_far()
    rb1[3].send_near()
    lower_rows(0, z)
    rb1[1].relay()
    ra1[2].relay()
    ra1[3].relay()
    rb1[2].relay()
    rb1[3].relay()

    def close_sum(pieces, n, sums, me):
        sums[near(me + order[n])] = pieces[n].finish().astype(BF16)

    close_sum(ra1, 0, a_sum, y)
    for piece in ra2:
        piece.send_far()
    close_sum(rb1, 0, b_sum, z)
    for piece in rb2:
        piece.send_far()
    for n in (1, 2):
        close_sum(ra1, n, a_sum, y)
        close_sum(rb1, n, b_sum, z)
    for piece in (*ra2, *rb2):
        piece.send_near()
    for piece in (*ra2, *rb2):
        piece.relay()
    close_sum(ra1, 3, a_sum, y)
    close_sum(rb1, 3, b_sum, z)

    first_back = net.take(len(across))
    backs = {step: first_back + n for n, step in enumerate(across)}
    for k, piece in enumerate((*ra2, *rb2)):
        so[k] = piece.finish().astype(BF16)
        for dc in range(2):
            core = lax.rem(c + dc, 2)
            mine = so.at[k, pl.ds(core * 16, 16)]
            if (k, dc) == (0, 0):
                rf[e, y] = mine[...]
            else:
                net.start(backs[k, dc], mine, rf.at[e, y], over_x(k, dc))

    out_pieces = [
        Gather(net, "batch", y, d, lambda b, k=k: rf.at[pl.ds(2 * near(x - k), 2), b])
        for k, d in enumerate((1, -1, 1, -1))
    ]
    for k, piece in enumerate(out_pieces):
        for dc in range(2):
            if (k, dc) != (0, 0):
                source = near(x - k) * 2 + lax.rem(c + dc, 2)
                net.arrived(backs[k, dc], rf.at[source, y], over_x(k, dc))
        piece.start()
    for piece in mix_pieces:
        piece.direct()
        piece.last()
    for piece in out_pieces:
        piece.relay()
    for piece in out_pieces:
        piece.direct()
    for piece in out_pieces:
        piece.last()

    @pl.loop(0, width // tile)
    def _(j):
        at = pl.ds(pl.multiple_of(j * tile, tile), tile)
        rows_in = rf[:, :, :, at].reshape(512, tile)
        mix = cb[...].reshape(RING * rows, 512)
        out[:, at] = jnp.dot(mix, rows_in, preferred_element_type=F32).astype(BF16)

    net.drain()


MESSAGES = 146


def local(tokens, gain, phi, w_gate, w_up, w_down):
    share = w_gate.shape[2]
    width = tokens.shape[2]
    count = tokens.shape[1]
    rows = count // RING
    slots = phi.shape[1]
    vmem = pltpu.VMEM
    scratch = [
        vmem((count, width), BF16),
        vmem((width, slots), BF16),
        vmem((D, share), BF16),
        vmem((D, share), BF16),
        vmem((share, D), BF16),
        vmem((count, width), BF16),
        vmem((RING, rows, slots), F32),
        vmem((3, 2, rows // 2, slots), F32),
        vmem((RING, 8, 128), F32),
        vmem((3, 8, 128), F32),
        vmem((RING, RING, 8, 128), F32),
        vmem((RING, rows, slots), BF16),
        vmem((RING, rows, slots), BF16),
        vmem((count, slots), BF16),
        vmem((8, RING, 16, width), BF16),
        vmem((3, 4, 2, 16, width), BF16),
        vmem((8, 16, width), BF16),
        vmem((RING, 2, RING, 64, width), BF16),
        vmem((share // 128, 2, 256, 256), F32),
        vmem((2, 256, share), BF16),
        vmem((RING, 2, RING, 64, width), BF16),
        vmem((3, 4, 64, width), BF16),
        vmem((RING, 64, width), BF16),
        vmem((3, 2, 32, width), BF16),
        vmem((3, 4, 64, width), BF16),
        vmem((RING, 64, width), BF16),
        vmem((3, 2, 32, width), BF16),
        vmem((4, 32, width), BF16),
        vmem((8, RING, 16, width), BF16),
        pltpu.SemaphoreType.DMA((5,)),
        pltpu.SemaphoreType.DMA((MESSAGES,)),
        pltpu.SemaphoreType.DMA((MESSAGES,)),
    ]
    anywhere = pl.BlockSpec(memory_space=pl.ANY)
    inside = pl.BlockSpec(memory_space=vmem)
    out = pl.pallas_call(
        kernel,
        out_shape=jax.ShapeDtypeStruct((count, width), BF16),
        in_specs=[anywhere, inside, anywhere, anywhere, anywhere, anywhere],
        out_specs=inside,
        scratch_shapes=scratch,
        compiler_params=pltpu.CompilerParams(
            collective_id=0, has_side_effects=True, vmem_limit_bytes=60 << 20
        ),
        name="soft_moe",
    )(tokens[0], gain[None], phi, w_gate[0], w_up[0], w_down[0])
    return out[None]


def solution(mesh):
    placed = (
        P("expert", "batch", "tensor"),
        P("tensor"),
        P("tensor", None),
        P("expert", None, ("batch", "tensor")),
        P("expert", None, ("batch", "tensor")),
        P("expert", ("batch", "tensor"), None),
    )
    return jax.shard_map(
        local, mesh=mesh, in_specs=placed, out_specs=P("expert", "batch", "tensor"), check_vma=False
    )
```

```python
import jax
import jax.numpy as jnp
from jax import lax
from jax.experimental import pallas as pl
from jax.experimental.pallas import tpu as pltpu
from jax.sharding import PartitionSpec as P


D = 4096
RING = 4
BF16 = jnp.bfloat16
F32 = jnp.float32


def near(v):
    return lax.rem(v + 2 * RING, RING)


class Net:
    def __init__(self, send_sems, recv_sems):
        self.send_sems, self.recv_sems = send_sems, recv_sems
        self.used, self.sent = 0, []

    def take(self, count=1):
        first = self.used
        self.used += count
        return first

    def copy(self, n, src, dst, target):
        return pltpu.make_async_remote_copy(
            src_ref=src,
            dst_ref=dst,
            send_sem=self.send_sems.at[n],
            recv_sem=self.recv_sems.at[n],
            device_id=target,
            device_id_type=pl.DeviceIdType.MESH,
        )

    def start(self, n, src, dst, target):
        one = self.copy(n, src, dst, target)
        one.start()
        self.sent.append(one)

    def arrived(self, n, dst, target):
        self.copy(n, dst, dst, target).wait_recv()

    def drain(self):
        for one in self.sent:
            one.wait_send()


class Gather:
    def __init__(self, net, axis, me, d, ref):
        self.net, self.axis, self.me, self.d, self.ref = net, axis, me, d, ref
        self.n = net.take(3)

    def to(self, d):
        return {self.axis: near(self.me + d)}

    def start(self):
        mine = self.ref(self.me)
        self.net.start(self.n, mine, mine, self.to(self.d))
        self.net.start(self.n + 1, mine, mine, self.to(-self.d))

    def relay(self):
        block = self.ref(near(self.me - self.d))
        self.net.arrived(self.n, block, self.to(self.d))
        self.net.start(self.n + 2, block, block, self.to(self.d))

    def direct(self):
        self.net.arrived(self.n + 1, self.ref(near(self.me + self.d)), self.to(self.d))

    def last(self):
        self.net.arrived(self.n + 2, self.ref(near(self.me + 2)), self.to(self.d))


class Scatter:
    def __init__(self, net, axis, me, d, part, buffers):
        self.net, self.axis, self.me, self.d, self.part = net, axis, me, d, part
        self.passing, self.direct_in, self.joined = buffers
        self.n = net.take(3)

    def to(self, d):
        return {self.axis: near(self.me + d)}

    def send_far(self):
        self.net.start(self.n, self.part(near(self.me + 2)), self.passing, self.to(self.d))

    def send_near(self):
        self.net.start(self.n + 1, self.part(near(self.me - self.d)), self.direct_in, self.to(-self.d))

    def relay(self):
        self.net.arrived(self.n, self.passing, self.to(self.d))
        term = self.part(near(self.me + self.d))
        total = term[...].astype(F32) + self.passing[...].astype(F32)
        term[...] = total.astype(term.dtype)
        self.net.start(self.n + 2, term, self.joined, self.to(self.d))

    def finish(self):
        self.net.arrived(self.n + 1, self.direct_in, self.to(self.d))
        self.net.arrived(self.n + 2, self.joined, self.to(self.d))
        mine = self.part(self.me)[...].astype(F32)
        return mine + self.direct_in[...].astype(F32) + self.joined[...].astype(F32)


def kernel(
    tok_in, gain, phi_in, wg_in, wu_in, wd_in, cb, rf,
    tok, phi, wg, wu, wd, tg,
    lp, l_in, sq_out, sq_in, st, qo, qg, qt,
    si, xs, acc, hid, ys,
    a_in, a_sum, a2_in, b_in, b_sum, b2_in, so,
    load_sems, send_sems, recv_sems,
):
    y = lax.axis_index("batch")
    e = lax.axis_index("expert")
    z = lax.axis_index("tensor")
    x, c = e // 2, lax.rem(e, 2)

    loads = [
        pltpu.make_async_copy(src, dst, load_sems.at[i])
        for i, (src, dst) in enumerate(
            ((tok_in, tok), (phi_in, phi), (wg_in, wg), (wu_in, wu), (wd_in, wd))
        )
    ]
    loads[0].start()
    loads[1].start()

    barrier = pltpu.get_barrier_semaphore()
    plane = [(dy, dz) for dy in range(RING) for dz in range(RING) if (dy, dz) != (0, 0)]
    across = [(dx, dc) for dx in (2, 1, 3, 0) for dc in range(2) if (dx, dc) != (0, 0)]

    def in_plane(dy, dz):
        return {"batch": near(y + dy), "tensor": near(z + dz)}

    def over_x(dx, dc):
        return {"expert": near(x + dx) * 2 + lax.rem(c + dc, 2)}

    peers = [in_plane(*step) for step in plane] + [over_x(*step) for step in across]
    for peer in peers:
        pl.semaphore_signal(
            barrier, inc=1, device_id=peer, device_id_type=pl.DeviceIdType.MESH
        )

    net = Net(send_sems, recv_sems)

    rows = lp.shape[1]
    width = tok.shape[1]
    wide = jnp.concatenate([gain[k : k + 1, :] for k in range(width // 128)], axis=1)
    loads[0].wait()
    tokens_f = tok[...].astype(F32)
    scaled = (tokens_f * wide.astype(F32)).astype(BF16)
    tg[y] = scaled
    squares = jnp.sum(tokens_f * tokens_f, axis=1, keepdims=True)
    diagonal = lax.broadcasted_iota(jnp.int32, (rows, 128), 0) == lax.broadcasted_iota(
        jnp.int32, (rows, 128), 1
    )
    for b in range(RING):
        column = squares[b * rows : (b + 1) * rows]
        line = jnp.sum(jnp.where(diagonal, column, 0.0), axis=0, keepdims=True)
        sq_out[b] = jnp.broadcast_to(line, (8, 128))
    loads[1].wait()
    for b in range(RING):
        part = jnp.dot(
            scaled[b * rows : (b + 1) * rows, :], phi[...], preferred_element_type=F32
        )
        lp[b] = part
    for one in loads[2:]:
        one.start()

    pl.semaphore_wait(barrier, len(peers))

    half = rows // 2
    logit_pieces = [
        Scatter(
            net, "tensor", z, d,
            lambda b, i=i: lp.at[b, pl.ds(i * half, half)],
            [l_in.at[k, i] for k in range(3)],
        )
        for i, d in enumerate((1, -1))
    ]
    token_pieces = [
        Gather(net, "batch", y, d, lambda b, i=i: tg.at[b, pl.ds(i * rows, rows)])
        for i, d in enumerate((1, -1, 1, -1))
    ]
    for piece in logit_pieces:
        piece.send_far()
    first_sq = net.take(3)
    for k in range(3):
        to = near(z + k + 1)
        net.start(first_sq + k, sq_out.at[to], sq_in.at[k], {"tensor": to})
    for piece in logit_pieces:
        piece.send_near()
    token_pieces[0].start()
    token_pieces[1].start()
    for piece in logit_pieces:
        piece.relay()
    token_pieces[2].start()
    for k in range(3):
        net.arrived(first_sq + k, sq_in.at[k], {"tensor": near(z + k + 1)})
    sq = sq_out[z] + sq_in[0] + sq_in[1] + sq_in[2]
    sq_column = jnp.sum(jnp.where(diagonal, sq[0:1, :], 0.0), axis=1, keepdims=True)
    inv_rms = lax.rsqrt(sq_column / D + 1e-06)
    logits = jnp.concatenate([piece.finish() for piece in logit_pieces], axis=0) * inv_rms

    lane = lax.broadcasted_iota(jnp.int32, (rows, 128), 1)
    quarters = []
    for q in range(RING):
        made = jnp.zeros((rows, 128), F32)
        for n in range(8):
            source = logits[:, n // 2 * 128 : n // 2 * 128 + 128]
            shift = (n * 16 - n % 2 * 64 - q * 16) % 128
            moved = pltpu.roll(source, shift, 1) if shift else source
            made = jnp.where((lane >= n * 16) & (lane < n * 16 + 16), moved, made)
        quarters.append(made)
    logits = jnp.concatenate(quarters, axis=1)

    local_max = jnp.max(logits, axis=0, keepdims=True)
    raised = jnp.exp(logits - local_max)
    local_total = jnp.sum(raised, axis=0, keepdims=True)
    mine = st.at[y, z]
    for k in range(RING):
        mine[k : k + 1, :] = local_max[:, k * 128 : (k + 1) * 128]
        mine[4 + k : 5 + k, :] = local_total[:, k * 128 : (k + 1) * 128]
    factor = (raised * inv_rms).astype(BF16)
    for k in range(RING):
        qo[k] = factor[:, k * 128 : (k + 1) * 128]
    qg[z, y] = qo[y]
    first_q = net.take(3)
    for k in (1, 0, 2):
        to = near(y + k + 1)
        net.start(first_q + k, qo.at[to], qg.at[z, y], {"batch": to})
    first_st = net.take(len(plane))
    for k, step in enumerate(plane):
        net.start(first_st + k, mine, mine, in_plane(*step))
    token_pieces[3].start()
    token_pieces[0].relay()
    token_pieces[1].relay()

    row_max = jnp.max(logits, axis=1, keepdims=True)
    row_raised = jnp.exp(logits - row_max)
    cb[z] = (row_raised / jnp.sum(row_raised, axis=1, keepdims=True)).astype(BF16)
    for k in range(3):
        net.arrived(first_q + k, qg.at[z, near(y - k - 1)], {"batch": near(y + k + 1)})
    q_pieces = [
        Gather(net, "tensor", z, d, lambda b, i=i: qg.at[b, pl.ds(i * 2, 2)])
        for i, d in enumerate((1, -1))
    ]
    for piece in q_pieces:
        piece.start()
    for k, (dy, dz) in enumerate(plane):
        net.arrived(first_st + k, st.at[near(y - dy), near(z - dz)], in_plane(dy, dz))
    maxima = st[:, :, pl.ds(y, 1), :]
    totals = st[:, :, pl.ds(RING + y, 1), :]
    top = jnp.max(jnp.max(maxima, axis=1, keepdims=True), axis=0, keepdims=True)
    weights = jnp.exp(maxima - top)
    total = jnp.sum(jnp.sum(totals * weights, axis=1, keepdims=True), axis=0, keepdims=True)
    weights = weights / total
    for piece in q_pieces:
        piece.relay()
    token_pieces[2].relay()
    token_pieces[3].relay()
    mix_pieces = [
        Gather(net, "tensor", z, d, lambda b, i=i: cb.at[b, pl.ds(i * half, half)])
        for i, d in enumerate((1, -1))
    ]
    for piece in q_pieces:
        piece.direct()
    for piece in q_pieces:
        piece.last()
    for b in range(RING):
        scaled_q = jnp.concatenate(
            [qg[k, b].astype(F32) * weights[b, k] for k in range(RING)], axis=0
        )
        qt[:, b * RING * rows : (b + 1) * RING * rows] = scaled_q.T.astype(BF16)
    for piece in token_pieces:
        piece.direct()
    for piece in token_pieces:
        piece.last()
    for piece in mix_pieces:
        piece.start()

    tile = 256
    for j in range(width // tile):
        at = pl.ds(j * tile, tile)
        part = jnp.dot(
            qt[...], tg[:, :, at].reshape(qt.shape[1], tile), preferred_element_type=F32
        )
        si[:, :, at] = part.astype(BF16).reshape(8, 16, tile)

    def place(k, core):
        return xs.at[z, k // 2, y, pl.ds(lax.rem(k, 2) * 32 + core * 16, 16)]

    first_x = net.take(len(across))
    for n, (dx, dc) in enumerate(across):
        target = over_x(dx, dc)
        net.start(
            first_x + n, si.at[target["expert"]], place((RING - dx) % RING, c), target
        )
    place(0, c)[...] = si[e]

    def wait_x(k):
        for n, (dx, dc) in enumerate(across):
            if (RING - dx) % RING == k:
                net.arrived(first_x + n, place(k, lax.rem(c + dc, 2)), over_x(dx, dc))

    a1 = [
        Gather(net, "batch", y, d, lambda b, i=i: xs.at[z, 0, b, pl.ds(i * 32, 32)])
        for i, d in enumerate((1, -1))
    ]
    b1 = [
        Gather(net, "tensor", z, d, lambda b, i=i: xs.at[b, 1, y, pl.ds(i * 32, 32)])
        for i, d in enumerate((1, -1))
    ]
    steps = (0, 3, 1, 2)
    ways = (1, 1, -1, -1)
    a2 = [
        Gather(net, "tensor", z, d, lambda b, j=j: xs.at[b, 0, near(y + j)])
        for j, d in zip(steps, ways)
    ]
    b2 = [
        Gather(net, "batch", y, d, lambda b, j=j: xs.at[near(z + j), 1, b])
        for j, d in zip(steps, ways)
    ]

    for k in (0, 1):
        wait_x(k)
        a1[k].start()
    for k in (2, 3):
        wait_x(k)
        b1[k - 2].start()
    for piece in mix_pieces:
        piece.relay()
    a2[0].start()
    b2[0].start()
    for stage in (a1, b1):
        for piece in stage:
            piece.relay()
    for stage, later in ((a1, a2), (b1, b2)):
        for piece in stage:
            piece.direct()
        later[1].start()
        later[2].start()
    for stage, later in ((a1, a2), (b1, b2)):
        for piece in stage:
            piece.last()
        later[3].start()

    loads[2].wait()
    loads[3].wait()
    share = acc.shape[0]

    def raise_rows(b, halves, first=False, last=False):
        deep = pl.ds(pl.multiple_of(b * width, width), width)
        lo, hi = halves[0], halves[-1] + 1
        count = (hi - lo) * RING * 64
        block = xs[b, lo:hi].reshape(count, width)
        for j in range(share):
            at = pl.ds(j * 128, 128)
            both = jnp.concatenate([wg[deep, at], wu[deep, at]], axis=1)
            part = jnp.dot(block, both, preferred_element_type=F32)
            if not first:
                part = acc[j, lo:hi].reshape(count, 256) + part
            if last:
                gate, up = part[:, :128], part[:, 128:]
                hid[:, at] = (gate / (1.0 + jnp.exp(-gate)) * up).astype(BF16)
            else:
                acc[j, lo:hi] = part.reshape(hi - lo, RING * 64, 256)

    raise_rows(z, (0,), first=True)
    a2[0].relay()
    b2[0].relay()
    a2[2].relay()
    b2[2].relay()
    b2[0].direct()
    a2[1].relay()
    b2[1].relay()
    b2[0].last()
    raise_rows(z, (1,), first=True)
    a2[3].relay()
    b2[3].relay()
    for piece in a2:
        piece.direct()
    b2[1].direct()
    b2[1].last()
    raise_rows(near(z - 1), (0, 1))
    b2[2].direct()
    b2[2].last()
    raise_rows(near(z + 1), (0, 1))
    for piece in a2:
        piece.last()
    b2[3].direct()
    b2[3].last()
    raise_rows(near(z + 2), (0, 1), last=True)

    loads[4].wait()

    def lower_rows(b):
        for j in range(width // tile):
            inside = pl.ds(j * tile, tile)
            at = pl.ds(pl.multiple_of(b * width + j * tile, tile), tile)
            part = jnp.dot(hid[...], wd[:, at], preferred_element_type=F32)
            ys[b, :, :, :, inside] = part.astype(BF16).reshape(2, RING, 64, tile)

    order = (2, 1, 3, 0)
    sides = (1, -1, 1, -1)
    ra1 = [
        Scatter(
            net, "tensor", z, d,
            lambda b, j=j: ys.at[b, 0, near(y + j)],
            [a_in.at[k, i] for k in range(3)],
        )
        for i, (j, d) in enumerate(zip(order, sides))
    ]
    rb1 = [
        Scatter(
            net, "batch", y, d,
            lambda b, j=j: ys.at[near(z + j), 1, b],
            [b_in.at[k, i] for k in range(3)],
        )
        for i, (j, d) in enumerate(zip(order, sides))
    ]
    ra2 = [
        Scatter(
            net, "batch", y, d,
            lambda b, i=i: a_sum.at[b, pl.ds(i * 32, 32)],
            [a2_in.at[k, i] for k in range(3)],
        )
        for i, d in enumerate((1, -1))
    ]
    rb2 = [
        Scatter(
            net, "tensor", z, d,
            lambda b, i=i: b_sum.at[b, pl.ds(i * 32, 32)],
            [b2_in.at[k, i] for k in range(3)],
        )
        for i, d in enumerate((1, -1))
    ]

    lower_rows(near(z + 2))
    for piece in ra1:
        piece.send_far()
    rb1[0].send_far()
    rb1[0].send_near()
    lower_rows(near(z + 1))
    ra1[1].send_near()
    ra1[3].send_near()
    rb1[1].send_far()
    rb1[1].send_near()
    lower_rows(near(z - 1))
    ra1[0].send_near()
    ra1[2].send_near()
    rb1[2].send_far()
    rb1[2].send_near()
    lower_rows(z)
    rb1[3].send_far()
    rb1[3].send_near()
    ra1[0].relay()
    ra1[1].relay()
    rb1[0].relay()
    rb1[1].relay()
    ra1[2].relay()
    ra1[3].relay()
    rb1[2].relay()
    rb1[3].relay()

    def close_sum(pieces, n, sums, me):
        sums[near(me + order[n])] = pieces[n].finish().astype(BF16)

    close_sum(ra1, 0, a_sum, y)
    for piece in ra2:
        piece.send_far()
    close_sum(rb1, 0, b_sum, z)
    for piece in rb2:
        piece.send_far()
    for n in (1, 2):
        close_sum(ra1, n, a_sum, y)
        close_sum(rb1, n, b_sum, z)
    for piece in (*ra2, *rb2):
        piece.send_near()
    for piece in (*ra2, *rb2):
        piece.relay()
    close_sum(ra1, 3, a_sum, y)
    close_sum(rb1, 3, b_sum, z)

    first_back = net.take(len(across))
    backs = {step: first_back + n for n, step in enumerate(across)}
    for k, piece in enumerate((*ra2, *rb2)):
        so[k] = piece.finish().astype(BF16)
        for dc in range(2):
            core = lax.rem(c + dc, 2)
            mine = so.at[k, pl.ds(core * 16, 16)]
            if (k, dc) == (0, 0):
                rf[y, e] = mine[...]
            else:
                net.start(backs[k, dc], mine, rf.at[y, e], over_x(k, dc))

    out_pieces = [
        Gather(net, "batch", y, d, lambda b, k=k: rf.at[b, pl.ds(2 * near(x - k), 2)])
        for k, d in enumerate((1, -1, 1, -1))
    ]
    for k, piece in enumerate(out_pieces):
        for dc in range(2):
            if (k, dc) != (0, 0):
                source = near(x - k) * 2 + lax.rem(c + dc, 2)
                net.arrived(backs[k, dc], rf.at[y, source], over_x(k, dc))
        piece.start()
    for piece in out_pieces:
        piece.relay()
    for piece in out_pieces:
        piece.direct()
    for piece in out_pieces:
        piece.last()

    for piece in mix_pieces:
        piece.direct()
        piece.last()
    net.drain()


MESSAGES = 149


def local(tokens, gain, phi, w_gate, w_up, w_down):
    share = w_gate.shape[2]
    width = tokens.shape[2]
    count = tokens.shape[1]
    rows = count // RING
    slots = phi.shape[1]
    vmem = pltpu.VMEM
    scratch = [
        vmem((count, width), BF16),
        vmem((width, slots), BF16),
        vmem((D, share), BF16),
        vmem((D, share), BF16),
        vmem((share, D), BF16),
        vmem((RING, count, width), BF16),
        vmem((RING, rows, slots), F32),
        vmem((3, 2, rows // 2, slots), F32),
        vmem((RING, 8, 128), F32),
        vmem((3, 8, 128), F32),
        vmem((RING, RING, 8, 128), F32),
        vmem((RING, rows, 128), BF16),
        vmem((RING, RING, rows, 128), BF16),
        vmem((128, RING * count), BF16),
        vmem((8, 16, width), BF16),
        vmem((RING, 2, RING, 64, width), BF16),
        vmem((share // 128, 2, 256, 256), F32),
        vmem((512, share), BF16),
        vmem((RING, 2, RING, 64, width), BF16),
        vmem((3, 4, 64, width), BF16),
        vmem((RING, 64, width), BF16),
        vmem((3, 2, 32, width), BF16),
        vmem((3, 4, 64, width), BF16),
        vmem((RING, 64, width), BF16),
        vmem((3, 2, 32, width), BF16),
        vmem((4, 32, width), BF16),
        pltpu.SemaphoreType.DMA((5,)),
        pltpu.SemaphoreType.DMA((MESSAGES,)),
        pltpu.SemaphoreType.DMA((MESSAGES,)),
    ]
    anywhere = pl.BlockSpec(memory_space=pl.ANY)
    inside = pl.BlockSpec(memory_space=vmem)
    mix, slot_rows = pl.pallas_call(
        kernel,
        out_shape=[
            jax.ShapeDtypeStruct((RING, rows, slots), BF16),
            jax.ShapeDtypeStruct((RING, 8, 16, width), BF16),
        ],
        in_specs=[anywhere, inside, anywhere, anywhere, anywhere, anywhere],
        out_specs=[inside, inside],
        scratch_shapes=scratch,
        compiler_params=pltpu.CompilerParams(
            collective_id=0, has_side_effects=True, vmem_limit_bytes=60 << 20
        ),
        name="soft_moe",
    )(tokens[0], gain.reshape(-1, 128), phi, w_gate[0], w_up[0], w_down[0])
    out = jnp.dot(
        mix.reshape(count, slots), slot_rows.reshape(slots, width), preferred_element_type=F32
    )
    return out.astype(BF16)[None]


def solution(mesh):
    placed = (
        P("expert", "batch", "tensor"),
        P("tensor"),
        P("tensor", None),
        P("expert", None, ("batch", "tensor")),
        P("expert", None, ("batch", "tensor")),
        P("expert", ("batch", "tensor"), None),
    )
    return jax.shard_map(
        local, mesh=mesh, in_specs=placed, out_specs=P("expert", "batch", "tensor"), check_vma=False
    )
```

```python
import jax
import jax.numpy as jnp
from jax import lax
from jax.experimental import pallas as pl
from jax.experimental.pallas import tpu as pltpu
from jax.sharding import PartitionSpec as P


D = 4096
RING = 4
BF16 = jnp.bfloat16
F32 = jnp.float32


def keep(v):
    return pltpu.with_memory_space_constraint(v, pltpu.HBM)


def near(v):
    return lax.rem(v + 2 * RING, RING)


class Net:
    def __init__(self, send_sems, recv_sems):
        self.send_sems, self.recv_sems = send_sems, recv_sems
        self.used, self.sent = 0, []

    def take(self, count=1):
        first = self.used
        self.used += count
        return first

    def copy(self, n, src, dst, target):
        return pltpu.make_async_remote_copy(
            src_ref=src,
            dst_ref=dst,
            send_sem=self.send_sems.at[n],
            recv_sem=self.recv_sems.at[n],
            device_id=target,
            device_id_type=pl.DeviceIdType.MESH,
        )

    def start(self, n, src, dst, target):
        one = self.copy(n, src, dst, target)
        one.start()
        self.sent.append(one)

    def arrived(self, n, dst, target):
        self.copy(n, dst, dst, target).wait_recv()

    def drain(self):
        for one in self.sent:
            one.wait_send()


class Gather:
    def __init__(self, net, axis, me, d, ref):
        self.net, self.axis, self.me, self.d, self.ref = net, axis, me, d, ref
        self.n = net.take(3)

    def to(self, d):
        return {self.axis: near(self.me + d)}

    def start(self):
        mine = self.ref(self.me)
        self.net.start(self.n, mine, mine, self.to(self.d))
        self.net.start(self.n + 1, mine, mine, self.to(-self.d))

    def relay(self):
        block = self.ref(near(self.me - self.d))
        self.net.arrived(self.n, block, self.to(self.d))
        self.net.start(self.n + 2, block, block, self.to(self.d))

    def direct(self):
        self.net.arrived(self.n + 1, self.ref(near(self.me + self.d)), self.to(self.d))

    def last(self):
        self.net.arrived(self.n + 2, self.ref(near(self.me + 2)), self.to(self.d))


class Scatter:
    def __init__(self, net, axis, me, d, part, buffers):
        self.net, self.axis, self.me, self.d, self.part = net, axis, me, d, part
        self.passing, self.direct_in, self.joined = buffers
        self.n = net.take(3)

    def to(self, d):
        return {self.axis: near(self.me + d)}

    def send_far(self):
        self.net.start(self.n, self.part(near(self.me + 2)), self.passing, self.to(self.d))

    def send_near(self):
        self.net.start(self.n + 1, self.part(near(self.me - self.d)), self.direct_in, self.to(-self.d))

    def relay(self):
        self.net.arrived(self.n, self.passing, self.to(self.d))
        term = self.part(near(self.me + self.d))
        total = term[...].astype(F32) + self.passing[...].astype(F32)
        term[...] = total.astype(term.dtype)
        self.net.start(self.n + 2, term, self.joined, self.to(self.d))

    def finish(self):
        self.net.arrived(self.n + 1, self.direct_in, self.to(self.d))
        self.net.arrived(self.n + 2, self.joined, self.to(self.d))
        mine = self.part(self.me)[...].astype(F32)
        return mine + self.direct_in[...].astype(F32) + self.joined[...].astype(F32)


def kernel(
    tok_in, gain, phi_in, wg_in, wu_in, wd_in, cb, rf,
    tok, phi, wg, wu, wd, tg,
    lp, l_in, sq_out, sq_in, st, qo, qg, qt,
    si, xs, acc, hid, ys,
    a_in, a_sum, a2_in, b_in, b_sum, b2_in, so,
    load_sems, send_sems, recv_sems,
):
    y = lax.axis_index("batch")
    e = lax.axis_index("expert")
    z = lax.axis_index("tensor")
    x, c = e // 2, lax.rem(e, 2)

    loads = [
        pltpu.make_async_copy(src, dst, load_sems.at[i])
        for i, (src, dst) in enumerate(
            ((tok_in, tok), (phi_in, phi), (wg_in, wg), (wu_in, wu), (wd_in, wd))
        )
    ]
    loads[0].start()
    loads[1].start()

    barrier = pltpu.get_barrier_semaphore()
    plane = [(dy, dz) for dy in range(RING) for dz in range(RING) if (dy, dz) != (0, 0)]
    across = [(dx, dc) for dx in (0, 1, 3, 2) for dc in range(2) if (dx, dc) != (0, 0)]

    def in_plane(dy, dz):
        return {"batch": near(y + dy), "tensor": near(z + dz)}

    def over_x(dx, dc):
        return {"expert": near(x + dx) * 2 + lax.rem(c + dc, 2)}

    peers = [in_plane(*step) for step in plane] + [over_x(*step) for step in across]
    for peer in peers:
        pl.semaphore_signal(
            barrier, inc=1, device_id=peer, device_id_type=pl.DeviceIdType.MESH
        )

    net = Net(send_sems, recv_sems)

    rows = lp.shape[1]
    width = tok.shape[1]
    wide = jnp.concatenate([gain[k : k + 1, :] for k in range(width // 128)], axis=1)
    loads[0].wait()
    tokens_f = tok[...].astype(F32)
    scaled = (tokens_f * wide.astype(F32)).astype(BF16)
    tg[y] = scaled
    squares = jnp.sum(tokens_f * tokens_f, axis=1, keepdims=True)
    diagonal = lax.broadcasted_iota(jnp.int32, (rows, 128), 0) == lax.broadcasted_iota(
        jnp.int32, (rows, 128), 1
    )
    for b in range(RING):
        column = squares[b * rows : (b + 1) * rows]
        line = jnp.sum(jnp.where(diagonal, column, 0.0), axis=0, keepdims=True)
        sq_out[b] = jnp.broadcast_to(line, (8, 128))
    loads[1].wait()
    for b in range(RING):
        part = jnp.dot(
            scaled[b * rows : (b + 1) * rows, :], phi[...], preferred_element_type=F32
        )
        lp[b] = part
    for one in loads[2:]:
        one.start()

    pl.semaphore_wait(barrier, len(peers))

    half = rows // 2
    logit_pieces = [
        Scatter(
            net, "tensor", z, d,
            lambda b, i=i: lp.at[b, pl.ds(i * half, half)],
            [l_in.at[k, i] for k in range(3)],
        )
        for i, d in enumerate((1, -1))
    ]
    token_pieces = [
        Gather(net, "batch", y, d, lambda b, i=i: tg.at[b, pl.ds(i * rows, rows)])
        for i, d in enumerate((1, -1, 1, -1))
    ]
    for piece in logit_pieces:
        piece.send_far()
    first_sq = net.take(3)
    for k in range(3):
        to = near(z + k + 1)
        net.start(first_sq + k, sq_out.at[to], sq_in.at[k], {"tensor": to})
    for piece in logit_pieces:
        piece.send_near()
    token_pieces[0].start()
    token_pieces[1].start()
    for piece in logit_pieces:
        piece.relay()
    token_pieces[2].start()
    for k in range(3):
        net.arrived(first_sq + k, sq_in.at[k], {"tensor": near(z + k + 1)})
    sq = sq_out[z] + sq_in[0] + sq_in[1] + sq_in[2]
    sq_column = jnp.sum(jnp.where(diagonal, sq[0:1, :], 0.0), axis=1, keepdims=True)
    inv_rms = lax.rsqrt(sq_column / D + 1e-06)
    logits = jnp.concatenate([piece.finish() for piece in logit_pieces], axis=0) * inv_rms

    lane = lax.broadcasted_iota(jnp.int32, (rows, 128), 1)
    quarters = []
    for q in range(RING):
        made = jnp.zeros((rows, 128), F32)
        for n in range(8):
            source = logits[:, n // 2 * 128 : n // 2 * 128 + 128]
            shift = (n * 16 - n % 2 * 64 - q * 16) % 128
            moved = pltpu.roll(source, shift, 1) if shift else source
            made = jnp.where((lane >= n * 16) & (lane < n * 16 + 16), moved, made)
        quarters.append(made)
    logits = jnp.concatenate(quarters, axis=1)

    local_max = jnp.max(logits, axis=0, keepdims=True)
    raised = jnp.exp(logits - local_max)
    local_total = jnp.sum(raised, axis=0, keepdims=True)
    mine = st.at[y, z]
    for k in range(RING):
        mine[k : k + 1, :] = local_max[:, k * 128 : (k + 1) * 128]
        mine[4 + k : 5 + k, :] = local_total[:, k * 128 : (k + 1) * 128]
    factor = (raised * inv_rms).astype(BF16)
    for k in range(RING):
        qo[k] = factor[:, k * 128 : (k + 1) * 128]
    qg[z, y] = qo[y]
    first_q = net.take(3)
    for k in (1, 0, 2):
        to = near(y + k + 1)
        net.start(first_q + k, qo.at[to], qg.at[z, y], {"batch": to})
    first_qz = net.take(12)

    def spread(k):
        block = qg.at[z, near(y - k)]
        for n in (0, 2, 1):
            net.start(first_qz + 3 * k + n, block, block, {"tensor": near(z + n + 1)})

    spread(0)
    first_st = net.take(len(plane))
    for k, step in enumerate(plane):
        net.start(first_st + k, mine, mine, in_plane(*step))
    token_pieces[3].start()
    token_pieces[0].relay()
    token_pieces[1].relay()

    row_max = jnp.max(logits, axis=1, keepdims=True)
    row_raised = jnp.exp(logits - row_max)
    cb[z] = (row_raised / jnp.sum(row_raised, axis=1, keepdims=True)).astype(BF16)
    mix_pieces = [
        Gather(net, "tensor", z, d, lambda b, i=i: cb.at[b, pl.ds(i * half, half)])
        for i, d in enumerate((1, -1))
    ]
    for piece in mix_pieces:
        piece.start()
    for k in (1, 3, 2):
        net.arrived(first_q + k - 1, qg.at[z, near(y - k)], {"batch": near(y + k)})
        spread(k)
        if k == 3:
            token_pieces[2].relay()
    token_pieces[3].relay()
    for k, (dy, dz) in enumerate(plane):
        net.arrived(first_st + k, st.at[near(y - dy), near(z - dz)], in_plane(dy, dz))
    maxima = st[:, :, pl.ds(y, 1), :]
    totals = st[:, :, pl.ds(RING + y, 1), :]
    top = jnp.max(jnp.max(maxima, axis=1, keepdims=True), axis=0, keepdims=True)
    weights = jnp.exp(maxima - top)
    total = jnp.sum(jnp.sum(totals * weights, axis=1, keepdims=True), axis=0, keepdims=True)
    weights = weights / total
    for piece in mix_pieces:
        piece.relay()
    for k in (0, 1, 3, 2):
        for n in range(3):
            net.arrived(
                first_qz + 3 * k + n,
                qg.at[near(z - n - 1), near(y - k)],
                {"tensor": near(z + n + 1)},
            )
    for b in range(RING):
        scaled_q = jnp.concatenate(
            [qg[k, b].astype(F32) * weights[b, k] for k in range(RING)], axis=0
        )
        qt[:, b * RING * rows : (b + 1) * RING * rows] = scaled_q.T.astype(BF16)
    for piece in token_pieces:
        piece.direct()
    for piece in token_pieces:
        piece.last()

    tile = 256
    for j in range(width // tile):
        at = pl.ds(j * tile, tile)
        part = jnp.dot(
            qt[...], tg[:, :, at].reshape(qt.shape[1], tile), preferred_element_type=F32
        )
        si[:, :, at] = part.astype(BF16).reshape(8, 16, tile)

    def place(k, core):
        return xs.at[z, k % 2, y, pl.ds(k // 2 * 32 + core * 16, 16)]

    first_x = net.take(len(across))
    for n, (dx, dc) in enumerate(across):
        target = over_x(dx, dc)
        net.start(
            first_x + n, si.at[target["expert"]], place((RING - dx) % RING, c), target
        )
    place(0, c)[...] = si[e]

    def wait_x(k):
        for n, (dx, dc) in enumerate(across):
            if (RING - dx) % RING == k:
                net.arrived(first_x + n, place(k, lax.rem(c + dc, 2)), over_x(dx, dc))

    a1 = [
        Gather(net, "batch", y, d, lambda b, i=i: xs.at[z, 0, b, pl.ds(i * 32, 32)])
        for i, d in enumerate((1, -1))
    ]
    b1 = [
        Gather(net, "tensor", z, d, lambda b, i=i: xs.at[b, 1, y, pl.ds(i * 32, 32)])
        for i, d in enumerate((1, -1))
    ]
    steps = (0, 3, 1, 2)
    ways = (1, 1, -1, -1)
    a2 = [
        Gather(net, "tensor", z, d, lambda b, j=j: xs.at[b, 0, near(y + j)])
        for j, d in zip(steps, ways)
    ]
    b2 = [
        Gather(net, "batch", y, d, lambda b, j=j: xs.at[near(z + j), 1, b])
        for j, d in zip(steps, ways)
    ]

    wait_x(0)
    a1[0].start()
    wait_x(1)
    b1[0].start()
    wait_x(3)
    b1[1].start()
    wait_x(2)
    a1[1].start()
    a2[0].start()
    b2[0].start()
    for stage in (a1, b1):
        for piece in stage:
            piece.relay()
    for stage, later in ((a1, a2), (b1, b2)):
        for piece in stage:
            piece.direct()
        later[1].start()
        later[2].start()
    for piece in a1:
        piece.last()
    a2[3].start()
    for piece in b1:
        piece.last()
    b2[0].relay()
    b2[3].start()

    loads[2].wait()
    loads[3].wait()
    share = acc.shape[0]

    def raise_rows(h, b, first=False, last=False):
        deep = pl.ds(pl.multiple_of(b * width, width), width)
        block = xs[b, h].reshape(RING * 64, width)
        for j in range(share):
            at = pl.ds(j * 128, 128)
            both = jnp.concatenate([wg[deep, at], wu[deep, at]], axis=1)
            part = jnp.dot(block, both, preferred_element_type=F32)
            if not first:
                part = acc[j, h] + part
            if last:
                gate, up = part[:, :128], part[:, 128:]
                hid[h, :, at] = (gate / (1.0 + jnp.exp(-gate)) * up).astype(BF16)
            else:
                acc[j, h] = part

    raise_rows(0, z, first=True)
    a2[0].relay()
    b2[1].relay()
    a2[1].relay()
    b2[2].relay()
    a2[2].relay()
    b2[0].direct()
    b2[0].last()
    raise_rows(1, z, first=True)
    for piece in a2:
        piece.direct()
    raise_rows(0, near(z - 1))
    b2[3].relay()
    a2[3].relay()
    raise_rows(0, near(z + 1))
    b2[2].direct()
    b2[2].last()
    raise_rows(1, near(z + 1))
    b2[1].direct()
    b2[1].last()
    raise_rows(1, near(z - 1))
    for piece in a2:
        piece.last()
    raise_rows(0, near(z + 2), last=True)

    loads[4].wait()

    def lower_rows(h, b):
        for j in range(width // tile):
            inside = pl.ds(j * tile, tile)
            at = pl.ds(pl.multiple_of(b * width + j * tile, tile), tile)
            part = jnp.dot(hid[h], wd[:, at], preferred_element_type=F32)
            ys[b, h, :, :, inside] = part.astype(BF16).reshape(RING, 64, tile)

    order = (2, 1, 3, 0)
    sides = (1, -1, 1, -1)
    ra1 = [
        Scatter(
            net, "tensor", z, d,
            lambda b, j=j: ys.at[b, 0, near(y + j)],
            [a_in.at[k, i] for k in range(3)],
        )
        for i, (j, d) in enumerate(zip(order, sides))
    ]
    rb1 = [
        Scatter(
            net, "batch", y, d,
            lambda b, j=j: ys.at[near(z + j), 1, b],
            [b_in.at[k, i] for k in range(3)],
        )
        for i, (j, d) in enumerate(zip(order, sides))
    ]
    ra2 = [
        Scatter(
            net, "batch", y, d,
            lambda b, i=i: a_sum.at[b, pl.ds(i * 32, 32)],
            [a2_in.at[k, i] for k in range(3)],
        )
        for i, d in enumerate((1, -1))
    ]
    rb2 = [
        Scatter(
            net, "tensor", z, d,
            lambda b, i=i: b_sum.at[b, pl.ds(i * 32, 32)],
            [b2_in.at[k, i] for k in range(3)],
        )
        for i, d in enumerate((1, -1))
    ]

    lower_rows(0, near(z + 2))
    for piece in ra1:
        piece.send_far()
    b2[3].direct()
    b2[3].last()
    raise_rows(1, near(z + 2), last=True)
    lower_rows(1, near(z + 2))
    rb1[0].send_far()
    rb1[0].send_near()
    lower_rows(1, near(z + 1))
    rb1[1].send_far()
    rb1[1].send_near()
    lower_rows(0, near(z + 1))
    ra1[1].send_near()
    ra1[3].send_near()
    lower_rows(0, near(z - 1))
    ra1[0].send_near()
    ra1[2].send_near()
    lower_rows(1, near(z - 1))
    rb1[2].send_far()
    rb1[2].send_near()
    ra1[0].relay()
    ra1[1].relay()
    lower_rows(1, z)
    rb1[3].send_far()
    rb1[3].send_near()
    rb1[0].relay()
    lower_rows(0, z)
    ra1[2].relay()
    ra1[3].relay()
    rb1[1].relay()
    rb1[2].relay()
    rb1[3].relay()

    def close_sum(pieces, n, sums, me):
        sums[near(me + order[n])] = pieces[n].finish().astype(BF16)

    both = ((ra1, a_sum, y, ra2), (rb1, b_sum, z, rb2))
    for stage, sums, me, later in both:
        close_sum(stage, 0, sums, me)
        later[0].send_far()
        later[1].send_far()
        close_sum(stage, 1, sums, me)
        later[1].send_near()
    for stage, sums, me, later in both:
        later[0].relay()
        close_sum(stage, 2, sums, me)
        later[0].send_near()
        later[1].relay()
    for stage, sums, me, later in both:
        close_sum(stage, 3, sums, me)

    first_back = net.take(len(across))
    backs = {step: first_back + n for n, step in enumerate(across)}
    for k, piece in ((1, rb2[0]), (3, rb2[1]), (2, ra2[1]), (0, ra2[0])):
        so[k] = piece.finish().astype(BF16)
        for dc in range(2):
            core = lax.rem(c + dc, 2)
            mine = so.at[k, pl.ds(core * 16, 16)]
            if (k, dc) == (0, 0):
                rf[y, e] = mine[...]
            else:
                net.start(backs[k, dc], mine, rf.at[y, e], over_x(k, dc))

    out_pieces = [
        Gather(net, "batch", y, d, lambda b, k=k: rf.at[b, pl.ds(2 * near(x - k), 2)])
        for k, d in enumerate((1, -1, 1, -1))
    ]
    for k in (0, 1, 3, 2):
        for dc in range(2):
            if (k, dc) != (0, 0):
                source = near(x - k) * 2 + lax.rem(c + dc, 2)
                net.arrived(backs[k, dc], rf.at[y, source], over_x(k, dc))
        out_pieces[k].start()
    for piece in out_pieces:
        piece.relay()
    for piece in out_pieces:
        piece.direct()
    for piece in out_pieces:
        piece.last()

    for piece in mix_pieces:
        piece.direct()
        piece.last()
    net.drain()


MESSAGES = 155


def local(tokens, gain, phi, w_gate, w_up, w_down):
    share = w_gate.shape[2]
    width = tokens.shape[2]
    count = tokens.shape[1]
    rows = count // RING
    slots = phi.shape[1]
    vmem = pltpu.VMEM
    scratch = [
        vmem((count, width), BF16),
        vmem((width, slots), BF16),
        vmem((D, share), BF16),
        vmem((D, share), BF16),
        vmem((share, D), BF16),
        vmem((RING, count, width), BF16),
        vmem((RING, rows, slots), F32),
        vmem((3, 2, rows // 2, slots), F32),
        vmem((RING, 8, 128), F32),
        vmem((3, 8, 128), F32),
        vmem((RING, RING, 8, 128), F32),
        vmem((RING, rows, 128), BF16),
        vmem((RING, RING, rows, 128), BF16),
        vmem((128, RING * count), BF16),
        vmem((8, 16, width), BF16),
        vmem((RING, 2, RING, 64, width), BF16),
        vmem((share // 128, 2, 256, 256), F32),
        vmem((2, 256, share), BF16),
        vmem((RING, 2, RING, 64, width), BF16),
        vmem((3, 4, 64, width), BF16),
        vmem((RING, 64, width), BF16),
        vmem((3, 2, 32, width), BF16),
        vmem((3, 4, 64, width), BF16),
        vmem((RING, 64, width), BF16),
        vmem((3, 2, 32, width), BF16),
        vmem((4, 32, width), BF16),
        pltpu.SemaphoreType.DMA((5,)),
        pltpu.SemaphoreType.DMA((MESSAGES,)),
        pltpu.SemaphoreType.DMA((MESSAGES,)),
    ]
    anywhere = pl.BlockSpec(memory_space=pltpu.HBM)
    inside = pl.BlockSpec(memory_space=vmem)
    mix, slot_rows = pl.pallas_call(
        kernel,
        out_shape=[
            jax.ShapeDtypeStruct((RING, rows, slots), BF16),
            jax.ShapeDtypeStruct((RING, 8, 16, width), BF16),
        ],
        in_specs=[anywhere, inside, anywhere, anywhere, anywhere, anywhere],
        out_specs=[inside, inside],
        scratch_shapes=scratch,
        compiler_params=pltpu.CompilerParams(
            collective_id=0, has_side_effects=True, vmem_limit_bytes=48 << 20
        ),
        name="soft_moe",
    )(keep(tokens[0]), keep(gain.reshape(-1, 128)), keep(phi), w_gate[0], w_up[0], w_down[0])
    out = jnp.dot(
        mix.reshape(count, slots), slot_rows.reshape(slots, width), preferred_element_type=F32
    )
    return out.astype(BF16)[None]


def solution(mesh):
    placed = (
        P("expert", "batch", "tensor"),
        P("tensor"),
        P("tensor", None),
        P("expert", None, ("batch", "tensor")),
        P("expert", None, ("batch", "tensor")),
        P("expert", ("batch", "tensor"), None),
    )
    return jax.shard_map(
        local, mesh=mesh, in_specs=placed, out_specs=P("expert", "batch", "tensor"), check_vma=False
    )
```

```python
import jax
import jax.numpy as jnp
from jax import lax
from jax.experimental import pallas as pl
from jax.experimental.pallas import tpu as pltpu
from jax.sharding import PartitionSpec as P


D = 4096
RING = 4
BF16 = jnp.bfloat16
F32 = jnp.float32


def keep(v):
    return pltpu.with_memory_space_constraint(v, pltpu.HBM)


def near(v):
    return lax.rem(v + 2 * RING, RING)


class Net:
    def __init__(self, send_sems, recv_sems):
        self.send_sems, self.recv_sems = send_sems, recv_sems
        self.used, self.sent = 0, []

    def take(self, count=1):
        first = self.used
        self.used += count
        return first

    def copy(self, n, src, dst, target):
        return pltpu.make_async_remote_copy(
            src_ref=src,
            dst_ref=dst,
            send_sem=self.send_sems.at[n],
            recv_sem=self.recv_sems.at[n],
            device_id=target,
            device_id_type=pl.DeviceIdType.MESH,
        )

    def start(self, n, src, dst, target):
        one = self.copy(n, src, dst, target)
        one.start()
        self.sent.append(one)

    def arrived(self, n, dst, target):
        self.copy(n, dst, dst, target).wait_recv()

    def drain(self):
        for one in self.sent:
            one.wait_send()


class Gather:
    def __init__(self, net, axis, me, d, ref):
        self.net, self.axis, self.me, self.d, self.ref = net, axis, me, d, ref
        self.n = net.take(3)

    def to(self, d):
        return {self.axis: near(self.me + d)}

    def start(self):
        mine = self.ref(self.me)
        self.net.start(self.n, mine, mine, self.to(self.d))
        self.net.start(self.n + 1, mine, mine, self.to(-self.d))

    def relay(self):
        block = self.ref(near(self.me - self.d))
        self.net.arrived(self.n, block, self.to(self.d))
        self.net.start(self.n + 2, block, block, self.to(self.d))

    def direct(self):
        self.net.arrived(self.n + 1, self.ref(near(self.me + self.d)), self.to(self.d))

    def last(self):
        self.net.arrived(self.n + 2, self.ref(near(self.me + 2)), self.to(self.d))


class Scatter:
    def __init__(self, net, axis, me, d, part, buffers):
        self.net, self.axis, self.me, self.d, self.part = net, axis, me, d, part
        self.passing, self.direct_in, self.joined = buffers
        self.n = net.take(3)

    def to(self, d):
        return {self.axis: near(self.me + d)}

    def send_far(self):
        self.net.start(self.n, self.part(near(self.me + 2)), self.passing, self.to(self.d))

    def send_near(self):
        self.net.start(self.n + 1, self.part(near(self.me - self.d)), self.direct_in, self.to(-self.d))

    def relay(self):
        self.net.arrived(self.n, self.passing, self.to(self.d))
        term = self.part(near(self.me + self.d))
        total = term[...].astype(F32) + self.passing[...].astype(F32)
        term[...] = total.astype(term.dtype)
        self.net.start(self.n + 2, term, self.joined, self.to(self.d))

    def finish(self):
        self.net.arrived(self.n + 1, self.direct_in, self.to(self.d))
        self.net.arrived(self.n + 2, self.joined, self.to(self.d))
        mine = self.part(self.me)[...].astype(F32)
        return mine + self.direct_in[...].astype(F32) + self.joined[...].astype(F32)


def kernel(
    tok_in, gain, phi_in, wg_in, wu_in, wd_in, cb, rf,
    tok, phi, wg, wu, wd, tg,
    lp, l_in, sq_out, sq_in, st, qo, qg, qt,
    si, xs, acc, hid, ys,
    a_in, a_sum, a2_in, b_in, b_sum, b2_in, so,
    load_sems, send_sems, recv_sems,
):
    y = lax.axis_index("batch")
    e = lax.axis_index("expert")
    z = lax.axis_index("tensor")
    x, c = e // 2, lax.rem(e, 2)

    loads = [
        pltpu.make_async_copy(src, dst, load_sems.at[i])
        for i, (src, dst) in enumerate(
            ((tok_in, tok), (phi_in, phi), (wg_in, wg), (wu_in, wu), (wd_in, wd))
        )
    ]
    loads[0].start()
    loads[1].start()

    barrier = pltpu.get_barrier_semaphore()
    plane = [(dy, dz) for dy in range(RING) for dz in range(RING) if (dy, dz) != (0, 0)]
    across = [(dx, dc) for dx in (0, 1, 3, 2) for dc in range(2) if (dx, dc) != (0, 0)]

    def in_plane(dy, dz):
        return {"batch": near(y + dy), "tensor": near(z + dz)}

    def over_x(dx, dc):
        return {"expert": near(x + dx) * 2 + lax.rem(c + dc, 2)}

    peers = [in_plane(*step) for step in plane] + [over_x(*step) for step in across]
    for peer in peers:
        pl.semaphore_signal(
            barrier, inc=1, device_id=peer, device_id_type=pl.DeviceIdType.MESH
        )

    net = Net(send_sems, recv_sems)

    rows = lp.shape[1]
    width = tok.shape[1]
    wide = jnp.concatenate([gain[k : k + 1, :] for k in range(width // 128)], axis=1)
    loads[0].wait()
    tokens_f = tok[...].astype(F32)
    scaled = (tokens_f * wide.astype(F32)).astype(BF16)
    tg[y] = scaled
    loads[1].wait()
    part = jnp.dot(scaled, phi[...], preferred_element_type=F32)
    lp[...] = part.reshape(lp.shape)
    for one in loads[2:]:
        one.start()

    pl.semaphore_wait(barrier, len(peers))

    half = rows // 2
    logit_pieces = [
        Scatter(
            net, "tensor", z, d,
            lambda b, i=i: lp.at[b, pl.ds(i * 16, 16)],
            [l_in.at[k, i] for k in range(3)],
        )
        for i, d in enumerate((1, -1, 1, -1))
    ]
    token_pieces = [
        Gather(net, "batch", y, d, lambda b, i=i: tg.at[b, :, pl.ds(i * 256, 256)])
        for i, d in enumerate((1, -1, 1, -1))
    ]
    for piece in logit_pieces:
        piece.send_far()
    for piece in logit_pieces:
        piece.send_near()
    token_pieces[0].start()
    token_pieces[1].start()

    squares = jnp.sum(tokens_f * tokens_f, axis=1, keepdims=True)
    diagonal = lax.broadcasted_iota(jnp.int32, (rows, 128), 0) == lax.broadcasted_iota(
        jnp.int32, (rows, 128), 1
    )
    for b in range(RING):
        column = squares[b * rows : (b + 1) * rows]
        line = jnp.sum(jnp.where(diagonal, column, 0.0), axis=0, keepdims=True)
        sq_out[b] = jnp.broadcast_to(line, (8, 128))
    first_sq = net.take(3)
    for k in range(3):
        to = near(z + k + 1)
        net.start(first_sq + k, sq_out.at[to], sq_in.at[k], {"tensor": to})
    for piece in logit_pieces:
        piece.relay()
    token_pieces[2].start()
    for k in range(3):
        net.arrived(first_sq + k, sq_in.at[k], {"tensor": near(z + k + 1)})
    sq = sq_out[z] + sq_in[0] + sq_in[1] + sq_in[2]
    sq_column = jnp.sum(jnp.where(diagonal, sq[0:1, :], 0.0), axis=1, keepdims=True)
    inv_rms = lax.rsqrt(sq_column / D + 1e-06)
    logits = jnp.concatenate([piece.finish() for piece in logit_pieces], axis=0) * inv_rms

    lane = lax.broadcasted_iota(jnp.int32, (rows, 128), 1)
    quarters = []
    for q in range(RING):
        made = jnp.zeros((rows, 128), F32)
        for n in range(8):
            source = logits[:, n // 2 * 128 : n // 2 * 128 + 128]
            shift = (n * 16 - n % 2 * 64 - q * 16) % 128
            moved = pltpu.roll(source, shift, 1) if shift else source
            made = jnp.where((lane >= n * 16) & (lane < n * 16 + 16), moved, made)
        quarters.append(made)
    logits = jnp.concatenate(quarters, axis=1)

    local_max = jnp.max(logits, axis=0, keepdims=True)
    raised = jnp.exp(logits - local_max)
    local_total = jnp.sum(raised, axis=0, keepdims=True)
    mine = st.at[y, z]
    for k in range(RING):
        mine[k : k + 1, :] = local_max[:, k * 128 : (k + 1) * 128]
        mine[4 + k : 5 + k, :] = local_total[:, k * 128 : (k + 1) * 128]
    factor = (raised * inv_rms).astype(BF16)
    for k in range(RING):
        qo[k] = factor[:, k * 128 : (k + 1) * 128]
    qg[z, y] = qo[y]
    first_q = net.take(3)
    for k in (1, 0, 2):
        to = near(y + k + 1)
        net.start(first_q + k, qo.at[to], qg.at[z, y], {"batch": to})
    first_qz = net.take(12)

    def spread(k):
        block = qg.at[z, near(y - k)]
        for n in (0, 2, 1):
            net.start(first_qz + 3 * k + n, block, block, {"tensor": near(z + n + 1)})

    spread(0)
    first_st = net.take(len(plane))
    for k, step in enumerate(plane):
        net.start(first_st + k, mine, mine, in_plane(*step))
    token_pieces[3].start()
    token_pieces[0].relay()
    token_pieces[1].relay()

    row_max = jnp.max(logits, axis=1, keepdims=True)
    row_raised = jnp.exp(logits - row_max)
    cb[z] = (row_raised / jnp.sum(row_raised, axis=1, keepdims=True)).astype(BF16)
    mix_pieces = [
        Gather(net, "tensor", z, d, lambda b, i=i: cb.at[b, pl.ds(i * half, half)])
        for i, d in enumerate((1, -1))
    ]
    for piece in mix_pieces:
        piece.start()
    for k in (1, 3, 2):
        net.arrived(first_q + k - 1, qg.at[z, near(y - k)], {"batch": near(y + k)})
        spread(k)
        if k == 3:
            token_pieces[2].relay()
    token_pieces[3].relay()
    for k, (dy, dz) in enumerate(plane):
        net.arrived(first_st + k, st.at[near(y - dy), near(z - dz)], in_plane(dy, dz))
    maxima = st[:, :, pl.ds(y, 1), :]
    totals = st[:, :, pl.ds(RING + y, 1), :]
    top = jnp.max(jnp.max(maxima, axis=1, keepdims=True), axis=0, keepdims=True)
    weights = jnp.exp(maxima - top)
    total = jnp.sum(jnp.sum(totals * weights, axis=1, keepdims=True), axis=0, keepdims=True)
    weights = weights / total
    for piece in mix_pieces:
        piece.relay()
    for k in (0, 1, 3, 2):
        for n in range(3):
            net.arrived(
                first_qz + 3 * k + n,
                qg.at[near(z - n - 1), near(y - k)],
                {"tensor": near(z + n + 1)},
            )
    for b in range(RING):
        scaled_q = jnp.concatenate(
            [qg[k, b].astype(F32) * weights[b, k] for k in range(RING)], axis=0
        )
        qt[:, b * RING * rows : (b + 1) * RING * rows] = scaled_q.T.astype(BF16)
    tile = 256

    def place(k, core, part):
        inside = pl.ds(k // 2 * 32 + core * 16, 16)
        return xs.at[z, k % 2, y, inside, pl.ds(part * 2 * tile, 2 * tile)]

    first_x = net.take(2 * len(across))
    for part in range(2):
        for piece in token_pieces[2 * part : 2 * part + 2]:
            piece.direct()
            piece.last()
        for j in (2 * part, 2 * part + 1):
            at = pl.ds(j * tile, tile)
            made = jnp.dot(
                qt[...], tg[:, :, at].reshape(qt.shape[1], tile), preferred_element_type=F32
            )
            si[:, :, at] = made.astype(BF16).reshape(8, 16, tile)
        own = pl.ds(part * 2 * tile, 2 * tile)
        for n, (dx, dc) in enumerate(across):
            target = over_x(dx, dc)
            net.start(
                first_x + 2 * n + part,
                si.at[target["expert"], :, own],
                place((RING - dx) % RING, c, part),
                target,
            )
        place(0, c, part)[...] = si[e, :, own]

    def wait_x(k):
        for n, (dx, dc) in enumerate(across):
            if (RING - dx) % RING == k:
                for part in range(2):
                    net.arrived(
                        first_x + 2 * n + part,
                        place(k, lax.rem(c + dc, 2), part),
                        over_x(dx, dc),
                    )

    a1 = [
        Gather(net, "batch", y, d, lambda b, i=i: xs.at[z, 0, b, pl.ds(i * 32, 32)])
        for i, d in enumerate((1, -1))
    ]
    b1 = [
        Gather(net, "tensor", z, d, lambda b, i=i: xs.at[b, 1, y, pl.ds(i * 32, 32)])
        for i, d in enumerate((1, -1))
    ]
    steps = (0, 3, 1, 2)
    ways = (1, 1, -1, -1)
    a2 = [
        Gather(net, "tensor", z, d, lambda b, j=j: xs.at[b, 0, near(y + j)])
        for j, d in zip(steps, ways)
    ]
    b2 = [
        Gather(net, "batch", y, d, lambda b, j=j: xs.at[near(z + j), 1, b])
        for j, d in zip(steps, ways)
    ]

    wait_x(0)
    a1[0].start()
    wait_x(1)
    b1[0].start()
    wait_x(3)
    b1[1].start()
    wait_x(2)
    a1[1].start()
    a2[0].start()
    b2[0].start()
    for stage in (a1, b1):
        for piece in stage:
            piece.relay()
    for stage, later in ((a1, a2), (b1, b2)):
        for piece in stage:
            piece.direct()
        later[1].start()
        later[2].start()
    for piece in a1:
        piece.last()
    a2[3].start()
    for piece in b1:
        piece.last()
    b2[0].relay()
    b2[3].start()

    loads[2].wait()
    loads[3].wait()
    share = acc.shape[0]

    def raise_rows(h, b, first=False, last=False):
        deep = pl.ds(pl.multiple_of(b * width, width), width)
        block = xs[b, h].reshape(RING * 64, width)
        for j in range(share):
            at = pl.ds(j * 128, 128)
            both = jnp.concatenate([wg[deep, at], wu[deep, at]], axis=1)
            part = jnp.dot(block, both, preferred_element_type=F32)
            if not first:
                part = acc[j, h] + part
            if last:
                gate, up = part[:, :128], part[:, 128:]
                hid[h, :, at] = (gate / (1.0 + jnp.exp(-gate)) * up).astype(BF16)
            else:
                acc[j, h] = part

    raise_rows(0, z, first=True)
    a2[0].relay()
    b2[1].relay()
    a2[1].relay()
    b2[2].relay()
    a2[2].relay()
    b2[0].direct()
    b2[0].last()
    raise_rows(1, z, first=True)
    for piece in a2:
        piece.direct()
    raise_rows(0, near(z - 1))
    b2[3].relay()
    a2[3].relay()
    raise_rows(0, near(z + 1))
    b2[2].direct()
    b2[2].last()
    raise_rows(1, near(z + 1))
    b2[1].direct()
    b2[1].last()
    raise_rows(1, near(z - 1))
    for piece in a2:
        piece.last()
    raise_rows(0, near(z + 2), last=True)

    loads[4].wait()

    def lower_rows(h, b):
        for j in range(width // tile):
            inside = pl.ds(j * tile, tile)
            at = pl.ds(pl.multiple_of(b * width + j * tile, tile), tile)
            part = jnp.dot(hid[h], wd[:, at], preferred_element_type=F32)
            ys[b, h, :, :, inside] = part.astype(BF16).reshape(RING, 64, tile)

    order = (2, 1, 3, 0)
    sides = (1, -1, 1, -1)
    ra1 = [
        Scatter(
            net, "tensor", z, d,
            lambda b, j=j: ys.at[b, 0, near(y + j)],
            [a_in.at[k, i] for k in range(3)],
        )
        for i, (j, d) in enumerate(zip(order, sides))
    ]
    rb1 = [
        Scatter(
            net, "batch", y, d,
            lambda b, j=j: ys.at[near(z + j), 1, b],
            [b_in.at[k, i] for k in range(3)],
        )
        for i, (j, d) in enumerate(zip(order, sides))
    ]
    minor = [(kk, dc) for kk in range(2) for dc in range(2)]

    def strip(kk, dc):
        return pl.ds(kk * 32 + lax.rem(c + dc, 2) * 16, 16)

    ra2 = [
        Scatter(
            net, "batch", y, 1 - 2 * dc,
            lambda b, kk=kk, dc=dc: a_sum.at[b, strip(kk, dc)],
            [a2_in.at[k, 2 * kk + dc] for k in range(3)],
        )
        for kk, dc in minor
    ]
    rb2 = [
        Scatter(
            net, "tensor", z, 1 - 2 * dc,
            lambda b, kk=kk, dc=dc: b_sum.at[b, strip(kk, dc)],
            [b2_in.at[k, 2 * kk + dc] for k in range(3)],
        )
        for kk, dc in minor
    ]

    lower_rows(0, near(z + 2))
    for piece in ra1:
        piece.send_far()
    b2[3].direct()
    b2[3].last()
    raise_rows(1, near(z + 2), last=True)
    lower_rows(1, near(z + 2))
    rb1[0].send_far()
    rb1[0].send_near()
    lower_rows(1, near(z + 1))
    rb1[1].send_far()
    rb1[1].send_near()
    lower_rows(0, near(z + 1))
    ra1[1].send_near()
    ra1[3].send_near()
    lower_rows(0, near(z - 1))
    ra1[0].send_near()
    ra1[2].send_near()
    lower_rows(1, near(z - 1))
    rb1[2].send_far()
    rb1[2].send_near()
    ra1[0].relay()
    ra1[1].relay()
    lower_rows(1, z)
    rb1[3].send_far()
    rb1[3].send_near()
    rb1[0].relay()
    lower_rows(0, z)
    ra1[2].relay()
    ra1[3].relay()
    rb1[1].relay()
    rb1[2].relay()
    rb1[3].relay()

    def close_sum(pieces, n, sums, me):
        sums[near(me + order[n])] = pieces[n].finish().astype(BF16)

    both = (
        (ra1, a_sum, y, (ra2[2], ra2[0]), (ra2[3], ra2[1])),
        (rb1, b_sum, z, (rb2[0], rb2[2]), (rb2[1], rb2[3])),
    )
    for stage, sums, me, plus, minus in both:
        close_sum(stage, 0, sums, me)
        for piece in (*plus, *minus):
            piece.send_far()
        close_sum(stage, 1, sums, me)
        for piece in minus:
            piece.send_near()
    for stage, sums, me, plus, minus in both:
        for piece in plus:
            piece.relay()
        close_sum(stage, 2, sums, me)
        for piece in plus:
            piece.send_near()
        for piece in minus:
            piece.relay()
    for stage, sums, me, plus, minus in both:
        close_sum(stage, 3, sums, me)

    first_back = net.take(len(across))
    backs = {step: first_back + n for n, step in enumerate(across)}
    for k, stage in ((1, rb2), (2, ra2), (3, rb2), (0, ra2)):
        for dc in range(2):
            done = stage[k // 2 * 2 + dc].finish().astype(BF16)
            if (k, dc) == (0, 0):
                rf[y, e] = done
            else:
                so[k, dc] = done
                net.start(backs[k, dc], so.at[k, dc], rf.at[y, e], over_x(k, dc))

    def source(k, dc):
        return near(x - k) * 2 + lax.rem(c + dc, 2)

    out_pieces = {
        (k, dc): Gather(
            net, "batch", y, 1 - 2 * dc, lambda b, k=k, dc=dc: rf.at[b, source(k, dc)]
        )
        for k in range(RING)
        for dc in range(2)
    }

    def start_out(k):
        for dc in range(2):
            if (k, dc) != (0, 0):
                net.arrived(backs[k, dc], rf.at[y, source(k, dc)], over_x(k, dc))
            out_pieces[k, dc].start()

    start_out(0)
    start_out(1)
    start_out(3)
    for dc in range(2):
        out_pieces[0, dc].relay()
    start_out(2)
    for k in (1, 3, 2):
        for dc in range(2):
            out_pieces[k, dc].relay()
    for piece in out_pieces.values():
        piece.direct()
    for piece in out_pieces.values():
        piece.last()

    for piece in mix_pieces:
        piece.direct()
        piece.last()
    net.drain()


MESSAGES = 192


def local(tokens, gain, phi, w_gate, w_up, w_down):
    share = w_gate.shape[2]
    width = tokens.shape[2]
    count = tokens.shape[1]
    rows = count // RING
    slots = phi.shape[1]
    vmem = pltpu.VMEM
    scratch = [
        vmem((count, width), BF16),
        vmem((width, slots), BF16),
        vmem((D, share), BF16),
        vmem((D, share), BF16),
        vmem((share, D), BF16),
        vmem((RING, count, width), BF16),
        vmem((RING, rows, slots), F32),
        vmem((3, 4, 16, slots), F32),
        vmem((RING, 8, 128), F32),
        vmem((3, 8, 128), F32),
        vmem((RING, RING, 8, 128), F32),
        vmem((RING, rows, 128), BF16),
        vmem((RING, RING, rows, 128), BF16),
        vmem((128, RING * count), BF16),
        vmem((8, 16, width), BF16),
        vmem((RING, 2, RING, 64, width), BF16),
        vmem((share // 128, 2, 256, 256), F32),
        vmem((2, 256, share), BF16),
        vmem((RING, 2, RING, 64, width), BF16),
        vmem((3, 4, 64, width), BF16),
        vmem((RING, 64, width), BF16),
        vmem((3, 4, 16, width), BF16),
        vmem((3, 4, 64, width), BF16),
        vmem((RING, 64, width), BF16),
        vmem((3, 4, 16, width), BF16),
        vmem((4, 2, 16, width), BF16),
        pltpu.SemaphoreType.DMA((5,)),
        pltpu.SemaphoreType.DMA((MESSAGES,)),
        pltpu.SemaphoreType.DMA((MESSAGES,)),
    ]
    anywhere = pl.BlockSpec(memory_space=pltpu.HBM)
    inside = pl.BlockSpec(memory_space=vmem)
    mix, slot_rows = pl.pallas_call(
        kernel,
        out_shape=[
            jax.ShapeDtypeStruct((RING, rows, slots), BF16),
            jax.ShapeDtypeStruct((RING, 8, 16, width), BF16),
        ],
        in_specs=[anywhere, inside, anywhere, anywhere, anywhere, anywhere],
        out_specs=[inside, inside],
        scratch_shapes=scratch,
        compiler_params=pltpu.CompilerParams(
            collective_id=0, has_side_effects=True, vmem_limit_bytes=48 << 20
        ),
        name="soft_moe",
    )(keep(tokens[0]), keep(gain.reshape(-1, 128)), keep(phi), w_gate[0], w_up[0], w_down[0])
    out = jnp.dot(
        mix.reshape(count, slots), slot_rows.reshape(slots, width), preferred_element_type=F32
    )
    return out.astype(BF16)[None]


def solution(mesh):
    placed = (
        P("expert", "batch", "tensor"),
        P("tensor"),
        P("tensor", None),
        P("expert", None, ("batch", "tensor")),
        P("expert", None, ("batch", "tensor")),
        P("expert", ("batch", "tensor"), None),
    )
    return jax.shard_map(
        local, mesh=mesh, in_specs=placed, out_specs=P("expert", "batch", "tensor"), check_vma=False
    )
```

```python
import jax
import jax.numpy as jnp
from jax import lax
from jax.experimental import pallas as pl
from jax.experimental.pallas import tpu as pltpu
from jax.sharding import PartitionSpec as P


D = 4096
RING = 4
BF16 = jnp.bfloat16
F32 = jnp.float32


def keep(v):
    return pltpu.with_memory_space_constraint(v, pltpu.HBM)


def near(v):
    return lax.rem(v + 2 * RING, RING)


class Net:
    def __init__(self, send_sems, recv_sems):
        self.send_sems, self.recv_sems = send_sems, recv_sems
        self.used, self.count, self.sent = 0, 0, {}

    def take(self, count):
        first = self.used
        self.used += count
        return first

    def copy(self, n, src, dst, target):
        return pltpu.make_async_remote_copy(
            src_ref=src,
            dst_ref=dst,
            send_sem=self.send_sems.at[self.count % SENDS],
            recv_sem=self.recv_sems.at[n],
            device_id=target,
            device_id_type=pl.DeviceIdType.MESH,
        )

    def start(self, n, src, dst, target):
        slot = self.count % SENDS
        if slot in self.sent:
            self.sent[slot].wait_send()
        one = self.copy(n, src, dst, target)
        one.start()
        self.sent[slot] = one
        self.count += 1

    def arrived(self, n, dst, target):
        self.copy(n, dst, dst, target).wait_recv()

    def drain(self):
        for one in self.sent.values():
            one.wait_send()


class Gather:
    def __init__(self, net, axis, me, d, ref):
        self.net, self.axis, self.me, self.d, self.ref = net, axis, me, d, ref
        self.n = net.take(3)

    def to(self, d):
        return {self.axis: near(self.me + d)}

    def start(self):
        mine = self.ref(self.me)
        self.net.start(self.n, mine, mine, self.to(self.d))
        self.net.start(self.n + 1, mine, mine, self.to(-self.d))

    def relay(self):
        block = self.ref(near(self.me - self.d))
        self.net.arrived(self.n, block, self.to(self.d))
        self.net.start(self.n + 2, block, block, self.to(self.d))

    def direct(self):
        self.net.arrived(self.n + 1, self.ref(near(self.me + self.d)), self.to(self.d))

    def last(self):
        self.net.arrived(self.n + 2, self.ref(near(self.me + 2)), self.to(self.d))


class Scatter:
    def __init__(self, net, axis, me, d, part, buffers):
        self.net, self.axis, self.me, self.d, self.part = net, axis, me, d, part
        self.passing, self.direct_in, self.joined = buffers
        self.n = net.take(3)

    def to(self, d):
        return {self.axis: near(self.me + d)}

    def send_far(self):
        self.net.start(self.n, self.part(near(self.me + 2)), self.passing, self.to(self.d))

    def send_near(self):
        self.net.start(self.n + 1, self.part(near(self.me - self.d)), self.direct_in, self.to(-self.d))

    def relay(self):
        self.net.arrived(self.n, self.passing, self.to(self.d))
        term = self.part(near(self.me + self.d))
        total = term[...].astype(F32) + self.passing[...].astype(F32)
        term[...] = total.astype(term.dtype)
        self.net.start(self.n + 2, term, self.joined, self.to(self.d))

    def finish(self):
        self.net.arrived(self.n + 1, self.direct_in, self.to(self.d))
        self.net.arrived(self.n + 2, self.joined, self.to(self.d))
        mine = self.part(self.me)[...].astype(F32)
        return mine + self.direct_in[...].astype(F32) + self.joined[...].astype(F32)


def kernel(
    tok_in, gain, phi_in, wg_in, wu_in, wd_in, cb, rf,
    tok, phi, wg, wu, wd, tg,
    lp, l_in, sq_out, sq_in, st, qo, qg, qt,
    si, xs, acc, hid, ys,
    a_in, a_sum, a2_in, b_in, b_sum, b2_in, so,
    load_sems, send_sems, recv_sems,
):
    y = lax.axis_index("batch")
    e = lax.axis_index("expert")
    z = lax.axis_index("tensor")
    x, c = e // 2, lax.rem(e, 2)

    loads = [
        pltpu.make_async_copy(src, dst, load_sems.at[i])
        for i, (src, dst) in enumerate(
            ((tok_in, tok), (phi_in, phi), (wg_in, wg), (wu_in, wu), (wd_in, wd))
        )
    ]
    loads[0].start()
    loads[1].start()

    barrier = pltpu.get_barrier_semaphore()
    plane = [(dy, dz) for dy in range(RING) for dz in range(RING) if (dy, dz) != (0, 0)]
    across = [(dx, dc) for dx in (0, 1, 3, 2) for dc in range(2) if (dx, dc) != (0, 0)]

    def in_plane(dy, dz):
        return {"batch": near(y + dy), "tensor": near(z + dz)}

    def over_x(dx, dc):
        return {"expert": near(x + dx) * 2 + lax.rem(c + dc, 2)}

    peers = [in_plane(*step) for step in plane] + [over_x(*step) for step in across]
    for peer in peers:
        pl.semaphore_signal(
            barrier, inc=1, device_id=peer, device_id_type=pl.DeviceIdType.MESH
        )

    net = Net(send_sems, recv_sems)

    rows = lp.shape[1]
    width = tok.shape[1]
    wide = jnp.concatenate([gain[k : k + 1, :] for k in range(width // 128)], axis=1)
    loads[0].wait()
    tokens_f = tok[...].astype(F32)
    scaled = (tokens_f * wide.astype(F32)).astype(BF16)
    tg[y] = scaled
    loads[1].wait()
    part = jnp.dot(scaled, phi[...], preferred_element_type=F32)
    lp[...] = part.reshape(lp.shape)
    for one in loads[2:]:
        one.start()

    pl.semaphore_wait(barrier, len(peers))

    half = rows // 2
    logit_pieces = [
        Scatter(
            net, "tensor", z, d,
            lambda b, i=i: lp.at[b, pl.ds(i * 16, 16)],
            [l_in.at[k, i] for k in range(3)],
        )
        for i, d in enumerate((1, -1, 1, -1))
    ]
    token_pieces = [
        Gather(net, "batch", y, d, lambda b, i=i: tg.at[b, :, pl.ds(i * 256, 256)])
        for i, d in enumerate((1, -1, 1, -1))
    ]
    for piece in logit_pieces:
        piece.send_far()
    for piece in logit_pieces:
        piece.send_near()
    token_pieces[0].start()
    token_pieces[1].start()

    squares = jnp.sum(tokens_f * tokens_f, axis=1, keepdims=True)
    diagonal = lax.broadcasted_iota(jnp.int32, (rows, 128), 0) == lax.broadcasted_iota(
        jnp.int32, (rows, 128), 1
    )
    for b in range(RING):
        column = squares[b * rows : (b + 1) * rows]
        line = jnp.sum(jnp.where(diagonal, column, 0.0), axis=0, keepdims=True)
        sq_out[b] = jnp.broadcast_to(line, (8, 128))
    first_sq = net.take(3)
    for k in range(3):
        to = near(z + k + 1)
        net.start(first_sq + k, sq_out.at[to], sq_in.at[k], {"tensor": to})
    for piece in logit_pieces:
        piece.relay()
    token_pieces[2].start()
    for k in range(3):
        net.arrived(first_sq + k, sq_in.at[k], {"tensor": near(z + k + 1)})
    sq = sq_out[z] + sq_in[0] + sq_in[1] + sq_in[2]
    sq_column = jnp.sum(jnp.where(diagonal, sq[0:1, :], 0.0), axis=1, keepdims=True)
    inv_rms = lax.rsqrt(sq_column / D + 1e-06)
    logits = jnp.concatenate([piece.finish() for piece in logit_pieces], axis=0) * inv_rms

    lane = lax.broadcasted_iota(jnp.int32, (rows, 128), 1)
    quarters = []
    for q in range(RING):
        made = jnp.zeros((rows, 128), F32)
        for n in range(8):
            source = logits[:, n // 2 * 128 : n // 2 * 128 + 128]
            shift = (n * 16 - n % 2 * 64 - q * 16) % 128
            moved = pltpu.roll(source, shift, 1) if shift else source
            made = jnp.where((lane >= n * 16) & (lane < n * 16 + 16), moved, made)
        quarters.append(made)
    logits = jnp.concatenate(quarters, axis=1)

    local_max = jnp.max(logits, axis=0, keepdims=True)
    raised = jnp.exp(logits - local_max)
    local_total = jnp.sum(raised, axis=0, keepdims=True)
    mine = st.at[y, z]
    for k in range(RING):
        mine[k : k + 1, :] = local_max[:, k * 128 : (k + 1) * 128]
        mine[4 + k : 5 + k, :] = local_total[:, k * 128 : (k + 1) * 128]
    factor = (raised * inv_rms).astype(BF16)
    for k in range(RING):
        qo[k] = factor[:, k * 128 : (k + 1) * 128]
    qg[z, y] = qo[y]
    first_q = net.take(3)
    for k in (1, 0, 2):
        to = near(y + k + 1)
        net.start(first_q + k, qo.at[to], qg.at[z, y], {"batch": to})
    first_qz = net.take(12)

    def spread(k):
        block = qg.at[z, near(y - k)]
        for n in (0, 2, 1):
            net.start(first_qz + 3 * k + n, block, block, {"tensor": near(z + n + 1)})

    spread(0)
    first_st = net.take(len(plane))
    for k, step in enumerate(plane):
        net.start(first_st + k, mine, mine, in_plane(*step))
    token_pieces[3].start()
    token_pieces[0].relay()
    token_pieces[1].relay()

    row_max = jnp.max(logits, axis=1, keepdims=True)
    row_raised = jnp.exp(logits - row_max)
    cb[z] = (row_raised / jnp.sum(row_raised, axis=1, keepdims=True)).astype(BF16)
    mix_pieces = [
        Gather(net, "tensor", z, d, lambda b, i=i: cb.at[b, pl.ds(i * half, half)])
        for i, d in enumerate((1, -1))
    ]
    for piece in mix_pieces:
        piece.start()
    for k in (1, 3, 2):
        net.arrived(first_q + k - 1, qg.at[z, near(y - k)], {"batch": near(y + k)})
        spread(k)
        if k == 3:
            token_pieces[2].relay()
    token_pieces[3].relay()
    for k, (dy, dz) in enumerate(plane):
        net.arrived(first_st + k, st.at[near(y - dy), near(z - dz)], in_plane(dy, dz))
    maxima = st[:, :, pl.ds(y, 1), :]
    totals = st[:, :, pl.ds(RING + y, 1), :]
    top = jnp.max(jnp.max(maxima, axis=1, keepdims=True), axis=0, keepdims=True)
    weights = jnp.exp(maxima - top)
    total = jnp.sum(jnp.sum(totals * weights, axis=1, keepdims=True), axis=0, keepdims=True)
    weights = weights / total
    for piece in mix_pieces:
        piece.relay()
    for k in (0, 1, 3, 2):
        for n in range(3):
            net.arrived(
                first_qz + 3 * k + n,
                qg.at[near(z - n - 1), near(y - k)],
                {"tensor": near(z + n + 1)},
            )
    for b in range(RING):
        scaled_q = jnp.concatenate(
            [qg[k, b].astype(F32) * weights[b, k] for k in range(RING)], axis=0
        )
        qt[:, b * RING * rows : (b + 1) * RING * rows] = scaled_q.T.astype(BF16)
    tile = 256

    def place(k, core, part):
        inside = pl.ds(k // 2 * 32 + core * 16, 16)
        return xs.at[z, k % 2, y, inside, pl.ds(part * 2 * tile, 2 * tile)]

    first_x = net.take(2 * len(across))
    for part in range(2):
        for piece in token_pieces[2 * part : 2 * part + 2]:
            piece.direct()
            piece.last()
        for j in (2 * part, 2 * part + 1):
            at = pl.ds(j * tile, tile)
            made = jnp.dot(
                qt[...], tg[:, :, at].reshape(qt.shape[1], tile), preferred_element_type=F32
            )
            si[:, :, at] = made.astype(BF16).reshape(8, 16, tile)
        own = pl.ds(part * 2 * tile, 2 * tile)
        for n, (dx, dc) in enumerate(across):
            target = over_x(dx, dc)
            net.start(
                first_x + 2 * n + part,
                si.at[target["expert"], :, own],
                place((RING - dx) % RING, c, part),
                target,
            )
        place(0, c, part)[...] = si[e, :, own]

    def wait_x(k):
        for n, (dx, dc) in enumerate(across):
            if (RING - dx) % RING == k:
                for part in range(2):
                    net.arrived(
                        first_x + 2 * n + part,
                        place(k, lax.rem(c + dc, 2), part),
                        over_x(dx, dc),
                    )

    fresh, net.used = net.used, 0
    a1 = [
        Gather(net, "batch", y, d, lambda b, i=i: xs.at[z, 0, b, pl.ds(i * 32, 32)])
        for i, d in enumerate((1, -1))
    ]
    b1 = [
        Gather(net, "tensor", z, d, lambda b, i=i: xs.at[b, 1, y, pl.ds(i * 32, 32)])
        for i, d in enumerate((1, -1))
    ]
    net.used = fresh
    low, high, whole = pl.ds(0, 32), pl.ds(32, 32), pl.ds(0, 64)
    cuts = ((0, low, 1), (0, high, -1), (3, whole, 1), (1, whole, -1), (2, low, 1), (2, high, -1))
    a2 = [
        Gather(net, "tensor", z, d, lambda b, j=j, r=r: xs.at[b, 0, near(y + j), r])
        for j, r, d in cuts
    ]
    b2 = [
        Gather(net, "batch", y, d, lambda b, j=j, r=r: xs.at[near(z + j), 1, b, r])
        for j, r, d in cuts
    ]

    wait_x(0)
    a1[0].start()
    a2[0].start()
    wait_x(1)
    b1[0].start()
    b2[0].start()
    wait_x(3)
    b1[1].start()
    wait_x(2)
    a1[1].start()
    b2[1].start()
    a2[1].start()
    for piece in (*a1, *b1):
        piece.relay()
    for stage, later in ((a1, a2), (b1, b2)):
        for piece in stage:
            piece.direct()
        later[2].start()
        later[3].start()
    for i in range(2):
        a1[i].last()
        a2[4 + i].start()
    b2[0].relay()
    b2[1].relay()
    for i in range(2):
        b1[i].last()
        b2[4 + i].start()
    for piece in mix_pieces:
        piece.direct()
        piece.last()

    loads[2].wait()
    loads[3].wait()
    share = acc.shape[0]

    def raise_rows(h, b, first=False, last=False):
        deep = pl.ds(pl.multiple_of(b * width, width), width)
        block = xs[b, h].reshape(RING * 64, width)
        for j in range(share):
            at = pl.ds(j * 128, 128)
            both = jnp.concatenate([wg[deep, at], wu[deep, at]], axis=1)
            part = jnp.dot(block, both, preferred_element_type=F32)
            if not first:
                part = acc[j, h] + part
            if last:
                gate, up = part[:, :128], part[:, 128:]
                hid[h, :, at] = (gate / (1.0 + jnp.exp(-gate)) * up).astype(BF16)
            else:
                acc[j, h] = part

    raise_rows(0, z, first=True)
    a2[0].relay()
    a2[1].relay()
    b2[2].relay()
    a2[2].relay()
    b2[3].relay()
    a2[3].relay()
    for piece in b2[:2]:
        piece.direct()
        piece.last()
    raise_rows(1, z, first=True)
    for piece in a2:
        piece.direct()
    a2[4].relay()
    a2[5].relay()
    raise_rows(0, near(z - 1))
    b2[4].relay()
    b2[5].relay()
    raise_rows(0, near(z + 1))
    b2[3].direct()
    b2[3].last()
    raise_rows(1, near(z + 1))
    b2[2].direct()
    b2[2].last()
    raise_rows(1, near(z - 1))
    for piece in a2:
        piece.last()
    raise_rows(0, near(z + 2), last=True)

    loads[4].wait()

    def lower_rows(h, b):
        for j in range(width // tile):
            inside = pl.ds(j * tile, tile)
            at = pl.ds(pl.multiple_of(b * width + j * tile, tile), tile)
            part = jnp.dot(hid[h], wd[:, at], preferred_element_type=F32)
            ys[b, h, :, :, inside] = part.astype(BF16).reshape(RING, 64, tile)

    order = (2, 1, 3, 0)
    sides = (1, -1, 1, -1)
    net.used = first_x
    ra1 = [
        Scatter(
            net, "tensor", z, d,
            lambda b, j=j: ys.at[b, 0, near(y + j)],
            [a_in.at[k, i] for k in range(3)],
        )
        for i, (j, d) in enumerate(zip(order, sides))
    ]
    net.used = 0
    rb1 = [
        Scatter(
            net, "batch", y, d,
            lambda b, j=j: ys.at[near(z + j), 1, b],
            [b_in.at[k, i] for k in range(3)],
        )
        for i, (j, d) in enumerate(zip(order, sides))
    ]
    net.used = token_pieces[0].n
    minor = [(kk, dc) for kk in range(2) for dc in range(2)]

    def strip(kk, dc):
        return pl.ds(kk * 32 + lax.rem(c + dc, 2) * 16, 16)

    ra2 = [
        Scatter(
            net, "batch", y, 1 - 2 * dc,
            lambda b, kk=kk, dc=dc: a_sum.at[b, strip(kk, dc)],
            [a2_in.at[k, 2 * kk + dc] for k in range(3)],
        )
        for kk, dc in minor
    ]
    rb2 = [
        Scatter(
            net, "tensor", z, 1 - 2 * dc,
            lambda b, kk=kk, dc=dc: b_sum.at[b, strip(kk, dc)],
            [b2_in.at[k, 2 * kk + dc] for k in range(3)],
        )
        for kk, dc in minor
    ]

    lower_rows(0, near(z + 2))
    for piece in ra1:
        piece.send_far()
    for piece in b2[4:]:
        piece.direct()
        piece.last()
    raise_rows(1, near(z + 2), last=True)
    lower_rows(1, near(z + 2))
    rb1[0].send_far()
    rb1[0].send_near()
    lower_rows(1, near(z + 1))
    rb1[1].send_far()
    rb1[1].send_near()
    lower_rows(0, near(z + 1))
    ra1[1].send_near()
    ra1[3].send_near()
    lower_rows(0, near(z - 1))
    ra1[0].send_near()
    ra1[2].send_near()
    lower_rows(1, near(z - 1))
    rb1[2].send_far()
    rb1[2].send_near()
    ra1[0].relay()
    ra1[1].relay()
    lower_rows(1, z)
    rb1[3].send_far()
    rb1[3].send_near()
    rb1[0].relay()
    lower_rows(0, z)
    ra1[2].relay()
    ra1[3].relay()
    rb1[1].relay()
    rb1[2].relay()
    rb1[3].relay()

    def close_sum(pieces, n, sums, me):
        sums[near(me + order[n])] = pieces[n].finish().astype(BF16)

    both = (
        (ra1, a_sum, y, (ra2[2], ra2[0]), (ra2[3], ra2[1])),
        (rb1, b_sum, z, (rb2[0], rb2[2]), (rb2[1], rb2[3])),
    )
    for stage, sums, me, plus, minus in both:
        close_sum(stage, 0, sums, me)
        for piece in (*plus, *minus):
            piece.send_far()
        close_sum(stage, 1, sums, me)
        for piece in minus:
            piece.send_near()
    for stage, sums, me, plus, minus in both:
        for piece in plus:
            piece.relay()
        close_sum(stage, 2, sums, me)
        for piece in plus:
            piece.send_near()
        for piece in minus:
            piece.relay()
    for stage, sums, me, plus, minus in both:
        close_sum(stage, 3, sums, me)

    first_back = net.take(len(across))
    backs = {step: first_back + n for n, step in enumerate(across)}
    for k, stage in ((1, rb2), (2, ra2), (3, rb2), (0, ra2)):
        for dc in range(2):
            done = stage[k // 2 * 2 + dc].finish().astype(BF16)
            if (k, dc) == (0, 0):
                rf[y, e] = done
            else:
                so[k, dc] = done
                net.start(backs[k, dc], so.at[k, dc], rf.at[y, e], over_x(k, dc))

    def source(k, dc):
        return near(x - k) * 2 + lax.rem(c + dc, 2)

    out_pieces = {
        (k, dc): Gather(
            net, "batch", y, 1 - 2 * dc, lambda b, k=k, dc=dc: rf.at[b, source(k, dc)]
        )
        for k in range(RING)
        for dc in range(2)
    }

    def start_out(k):
        for dc in range(2):
            if (k, dc) != (0, 0):
                net.arrived(backs[k, dc], rf.at[y, source(k, dc)], over_x(k, dc))
            out_pieces[k, dc].start()

    start_out(0)
    start_out(1)
    start_out(3)
    for dc in range(2):
        out_pieces[0, dc].relay()
    start_out(2)
    for k in (1, 3, 2):
        for dc in range(2):
            out_pieces[k, dc].relay()
    for piece in out_pieces.values():
        piece.direct()
    for piece in out_pieces.values():
        piece.last()

    net.drain()


SENDS, ARRIVALS = 40, 113


def local(tokens, gain, phi, w_gate, w_up, w_down):
    share = w_gate.shape[2]
    width = tokens.shape[2]
    count = tokens.shape[1]
    rows = count // RING
    slots = phi.shape[1]
    vmem = pltpu.VMEM
    scratch = [
        vmem((count, width), BF16),
        vmem((width, slots), BF16),
        vmem((D, share), BF16),
        vmem((D, share), BF16),
        vmem((share, D), BF16),
        vmem((RING, count, width), BF16),
        vmem((RING, rows, slots), F32),
        vmem((3, 4, 16, slots), F32),
        vmem((RING, 8, 128), F32),
        vmem((3, 8, 128), F32),
        vmem((RING, RING, 8, 128), F32),
        vmem((RING, rows, 128), BF16),
        vmem((RING, RING, rows, 128), BF16),
        vmem((128, RING * count), BF16),
        vmem((8, 16, width), BF16),
        vmem((RING, 2, RING, 64, width), BF16),
        vmem((share // 128, 2, 256, 256), F32),
        vmem((2, 256, share), BF16),
        vmem((RING, 2, RING, 64, width), BF16),
        vmem((3, 4, 64, width), BF16),
        vmem((RING, 64, width), BF16),
        vmem((3, 4, 16, width), BF16),
        vmem((3, 4, 64, width), BF16),
        vmem((RING, 64, width), BF16),
        vmem((3, 4, 16, width), BF16),
        vmem((4, 2, 16, width), BF16),
        pltpu.SemaphoreType.DMA((5,)),
        pltpu.SemaphoreType.DMA((SENDS,)),
        pltpu.SemaphoreType.DMA((ARRIVALS,)),
    ]
    anywhere = pl.BlockSpec(memory_space=pltpu.HBM)
    inside = pl.BlockSpec(memory_space=vmem)
    mix, slot_rows = pl.pallas_call(
        kernel,
        out_shape=[
            jax.ShapeDtypeStruct((RING, rows, slots), BF16),
            jax.ShapeDtypeStruct((RING, 8, 16, width), BF16),
        ],
        in_specs=[anywhere, inside, anywhere, anywhere, anywhere, anywhere],
        out_specs=[inside, inside],
        scratch_shapes=scratch,
        compiler_params=pltpu.CompilerParams(
            collective_id=0, has_side_effects=True, vmem_limit_bytes=48 << 20
        ),
        name="soft_moe",
    )(keep(tokens[0]), keep(gain.reshape(-1, 128)), keep(phi), w_gate[0], w_up[0], w_down[0])
    out = jnp.dot(
        mix.reshape(count, slots), slot_rows.reshape(slots, width), preferred_element_type=F32
    )
    return out.astype(BF16)[None]


def solution(mesh):
    placed = (
        P("expert", "batch", "tensor"),
        P("tensor"),
        P("tensor", None),
        P("expert", None, ("batch", "tensor")),
        P("expert", None, ("batch", "tensor")),
        P("expert", ("batch", "tensor"), None),
    )
    return jax.shard_map(
        local, mesh=mesh, in_specs=placed, out_specs=P("expert", "batch", "tensor"), check_vma=False
    )
```

```python
import jax
import jax.numpy as jnp
from jax import lax
from jax.experimental import pallas as pl
from jax.experimental.pallas import tpu as pltpu
from jax.sharding import PartitionSpec as P


D = 4096
RING = 4
BF16 = jnp.bfloat16
F32 = jnp.float32


def keep(v):
    return pltpu.with_memory_space_constraint(v, pltpu.HBM)


def near(v):
    return lax.rem(v + 2 * RING, RING)


class Net:
    def __init__(self, send_sems, recv_sems):
        self.send_sems, self.recv_sems = send_sems, recv_sems
        self.used, self.count, self.sent = 0, 0, {}

    def take(self, count):
        first = self.used
        self.used += count
        return first

    def copy(self, n, src, dst, target):
        return pltpu.make_async_remote_copy(
            src_ref=src,
            dst_ref=dst,
            send_sem=self.send_sems.at[self.count % SENDS],
            recv_sem=self.recv_sems.at[n],
            device_id=target,
            device_id_type=pl.DeviceIdType.MESH,
        )

    def start(self, n, src, dst, target):
        slot = self.count % SENDS
        if slot in self.sent:
            self.sent[slot].wait_send()
        one = self.copy(n, src, dst, target)
        one.start()
        self.sent[slot] = one
        self.count += 1

    def arrived(self, n, dst, target):
        self.copy(n, dst, dst, target).wait_recv()

    def drain(self):
        for one in self.sent.values():
            one.wait_send()


class Gather:
    def __init__(self, net, axis, me, d, ref):
        self.net, self.axis, self.me, self.d, self.ref = net, axis, me, d, ref
        self.n = net.take(3)

    def to(self, d):
        return {self.axis: near(self.me + d)}

    def start(self):
        mine = self.ref(self.me)
        self.net.start(self.n, mine, mine, self.to(self.d))
        self.net.start(self.n + 1, mine, mine, self.to(-self.d))

    def relay(self):
        block = self.ref(near(self.me - self.d))
        self.net.arrived(self.n, block, self.to(self.d))
        self.net.start(self.n + 2, block, block, self.to(self.d))

    def direct(self):
        self.net.arrived(self.n + 1, self.ref(near(self.me + self.d)), self.to(self.d))

    def last(self):
        self.net.arrived(self.n + 2, self.ref(near(self.me + 2)), self.to(self.d))


class Scatter:
    def __init__(self, net, axis, me, d, part, buffers):
        self.net, self.axis, self.me, self.d, self.part = net, axis, me, d, part
        self.passing, self.direct_in, self.joined = buffers
        self.n = net.take(3)

    def to(self, d):
        return {self.axis: near(self.me + d)}

    def send_far(self):
        self.net.start(self.n, self.part(near(self.me + 2)), self.passing, self.to(self.d))

    def send_near(self):
        self.net.start(self.n + 1, self.part(near(self.me - self.d)), self.direct_in, self.to(-self.d))

    def relay(self):
        self.net.arrived(self.n, self.passing, self.to(self.d))
        term = self.part(near(self.me + self.d))
        total = term[...].astype(F32) + self.passing[...].astype(F32)
        term[...] = total.astype(term.dtype)
        self.net.start(self.n + 2, term, self.joined, self.to(self.d))

    def finish(self):
        self.net.arrived(self.n + 1, self.direct_in, self.to(self.d))
        self.net.arrived(self.n + 2, self.joined, self.to(self.d))
        mine = self.part(self.me)[...].astype(F32)
        return mine + self.direct_in[...].astype(F32) + self.joined[...].astype(F32)


def kernel(
    tok_in, gain, phi_in, wg_in, wu_in, wd_in, cb, rf,
    tok, phi, wg, wu, wd, tg,
    lp, l_in, sq_out, sq_in, sx, st, qo, qg, qt,
    si, xs, acc, hid, ys,
    a_in, a_sum, a2_in, b_in, b_sum, b2_in, so,
    load_sems, send_sems, recv_sems,
):
    y = lax.axis_index("batch")
    e = lax.axis_index("expert")
    z = lax.axis_index("tensor")
    x, c = e // 2, lax.rem(e, 2)

    loads = [
        pltpu.make_async_copy(src, dst, load_sems.at[i])
        for i, (src, dst) in enumerate(
            ((tok_in, tok), (phi_in, phi), (wg_in, wg), (wu_in, wu), (wd_in, wd))
        )
    ]
    loads[0].start()
    loads[1].start()

    barrier = pltpu.get_barrier_semaphore()
    plane = [(dy, dz) for dy in range(RING) for dz in range(RING) if (dy, dz) != (0, 0)]
    across = [(dx, dc) for dx in (0, 1, 3, 2) for dc in range(2) if (dx, dc) != (0, 0)]

    def in_plane(dy, dz):
        return {"batch": near(y + dy), "tensor": near(z + dz)}

    def over_x(dx, dc):
        return {"expert": near(x + dx) * 2 + lax.rem(c + dc, 2)}

    peers = [in_plane(*step) for step in plane] + [over_x(*step) for step in across]
    for peer in peers:
        pl.semaphore_signal(
            barrier, inc=1, device_id=peer, device_id_type=pl.DeviceIdType.MESH
        )

    net = Net(send_sems, recv_sems)

    rows = lp.shape[1]
    width = tok.shape[1]
    wide = jnp.concatenate([gain[k : k + 1, :] for k in range(width // 128)], axis=1)
    loads[0].wait()
    tokens_f = tok[...].astype(F32)
    scaled = (tokens_f * wide.astype(F32)).astype(BF16)
    tg[y] = scaled
    loads[1].wait()
    part = jnp.dot(scaled, phi[...], preferred_element_type=F32)
    lp[...] = part.reshape(lp.shape)
    for one in loads[2:]:
        one.start()

    pl.semaphore_wait(barrier, len(peers))

    half = rows // 2
    logit_pieces = [
        Scatter(
            net, "tensor", z, d,
            lambda b, i=i: lp.at[b, pl.ds(i * 16, 16)],
            [l_in.at[k, i] for k in range(3)],
        )
        for i, d in enumerate((1, -1, 1, -1))
    ]
    token_pieces = [
        Gather(net, "batch", y, d, lambda b, i=i: tg.at[b, :, pl.ds(i * 256, 256)])
        for i, d in enumerate((1, -1, 1, -1))
    ]
    for piece in logit_pieces:
        piece.send_far()
    for piece in logit_pieces:
        piece.send_near()
    token_pieces[0].start()
    token_pieces[1].start()

    squares = jnp.sum(tokens_f * tokens_f, axis=1, keepdims=True)
    diagonal = lax.broadcasted_iota(jnp.int32, (rows, 128), 0) == lax.broadcasted_iota(
        jnp.int32, (rows, 128), 1
    )
    for b in range(RING):
        column = squares[b * rows : (b + 1) * rows]
        line = jnp.sum(jnp.where(diagonal, column, 0.0), axis=0, keepdims=True)
        sq_out[b] = jnp.broadcast_to(line, (8, 128))
    first_sq = net.take(3)
    for k in range(3):
        to = near(z + k + 1)
        net.start(first_sq + k, sq_out.at[to], sq_in.at[k], {"tensor": to})
    for piece in logit_pieces:
        piece.relay()
    token_pieces[2].start()
    for k in range(3):
        net.arrived(first_sq + k, sq_in.at[k], {"tensor": near(z + k + 1)})
    sq = sq_out[z] + sq_in[0] + sq_in[1] + sq_in[2]
    sq_column = jnp.sum(jnp.where(diagonal, sq[0:1, :], 0.0), axis=1, keepdims=True)
    inv_rms = lax.rsqrt(sq_column / D + 1e-06)
    logits = jnp.concatenate([piece.finish() for piece in logit_pieces], axis=0) * inv_rms

    lane = lax.broadcasted_iota(jnp.int32, (rows, 128), 1)
    quarters = []
    for q in range(RING):
        made = jnp.zeros((rows, 128), F32)
        for n in range(8):
            source = logits[:, n // 2 * 128 : n // 2 * 128 + 128]
            shift = (n * 16 - n % 2 * 64 - q * 16) % 128
            moved = pltpu.roll(source, shift, 1) if shift else source
            made = jnp.where((lane >= n * 16) & (lane < n * 16 + 16), moved, made)
        quarters.append(made)
    logits = jnp.concatenate(quarters, axis=1)

    local_max = jnp.max(logits, axis=0, keepdims=True)
    raised = jnp.exp(logits - local_max)
    local_total = jnp.sum(raised, axis=0, keepdims=True)
    for k in range(RING):
        sx[k, 0:1, :] = local_max[:, k * 128 : (k + 1) * 128]
        sx[k, 1:2, :] = local_total[:, k * 128 : (k + 1) * 128]
    st[y, z] = sx[y]
    factor = (raised * inv_rms).astype(BF16)
    for k in range(RING):
        qo[k] = factor[:, k * 128 : (k + 1) * 128]
    qg[z, y] = qo[y]
    first_q = net.take(3)
    for k in (1, 0, 2):
        to = near(y + k + 1)
        net.start(first_q + k, qo.at[to], qg.at[z, y], {"batch": to})
    first_qz = net.take(12)

    def spread(k):
        block = qg.at[z, near(y - k)]
        for n in (0, 2, 1):
            net.start(first_qz + 3 * k + n, block, block, {"tensor": near(z + n + 1)})

    spread(0)
    first_st = net.take(len(plane))
    for k, step in enumerate(plane):
        net.start(first_st + k, sx.at[near(y + step[0])], st.at[y, z], in_plane(*step))
    token_pieces[3].start()
    token_pieces[0].relay()
    token_pieces[1].relay()

    row_max = jnp.max(logits, axis=1, keepdims=True)
    row_raised = jnp.exp(logits - row_max)
    cb[z] = (row_raised / jnp.sum(row_raised, axis=1, keepdims=True)).astype(BF16)
    mix_pieces = [
        Gather(net, "tensor", z, d, lambda b, i=i: cb.at[b, pl.ds(i * half, half)])
        for i, d in enumerate((1, -1))
    ]
    for piece in mix_pieces:
        piece.start()
    for k in (1, 3, 2):
        net.arrived(first_q + k - 1, qg.at[z, near(y - k)], {"batch": near(y + k)})
        spread(k)
        if k == 3:
            token_pieces[2].relay()
    token_pieces[3].relay()
    for k, (dy, dz) in enumerate(plane):
        net.arrived(first_st + k, st.at[near(y - dy), near(z - dz)], in_plane(dy, dz))
    maxima = st[:, :, 0:1, :]
    totals = st[:, :, 1:2, :]
    top = jnp.max(jnp.max(maxima, axis=1, keepdims=True), axis=0, keepdims=True)
    weights = jnp.exp(maxima - top)
    total = jnp.sum(jnp.sum(totals * weights, axis=1, keepdims=True), axis=0, keepdims=True)
    weights = weights / total
    for piece in mix_pieces:
        piece.relay()
    for k in (0, 1, 3, 2):
        for n in range(3):
            net.arrived(
                first_qz + 3 * k + n,
                qg.at[near(z - n - 1), near(y - k)],
                {"tensor": near(z + n + 1)},
            )
    for b in range(RING):
        scaled_q = jnp.concatenate(
            [qg[k, b].astype(F32) * weights[b, k] for k in range(RING)], axis=0
        )
        qt[:, b * RING * rows : (b + 1) * RING * rows] = scaled_q.T.astype(BF16)
    tile = 256

    def place(k, core, part):
        inside = pl.ds(k // 2 * 32 + core * 16, 16)
        return xs.at[z, (k + 1) % 2, y, inside, pl.ds(part * 2 * tile, 2 * tile)]

    first_x = net.take(2 * len(across))
    for part in range(2):
        for piece in token_pieces[2 * part : 2 * part + 2]:
            piece.direct()
            piece.last()
        for j in (2 * part, 2 * part + 1):
            at = pl.ds(j * tile, tile)
            made = jnp.dot(
                qt[...], tg[:, :, at].reshape(qt.shape[1], tile), preferred_element_type=F32
            )
            si[:, :, at] = made.astype(BF16).reshape(8, 16, tile)
        own = pl.ds(part * 2 * tile, 2 * tile)
        for n, (dx, dc) in enumerate(across):
            target = over_x(dx, dc)
            net.start(
                first_x + 2 * n + part,
                si.at[target["expert"], :, own],
                place((RING - dx) % RING, c, part),
                target,
            )
        place(0, c, part)[...] = si[e, :, own]

    def wait_x(k):
        for n, (dx, dc) in enumerate(across):
            if (RING - dx) % RING == k:
                for part in range(2):
                    net.arrived(
                        first_x + 2 * n + part,
                        place(k, lax.rem(c + dc, 2), part),
                        over_x(dx, dc),
                    )

    fresh, net.used = net.used, 0
    a1 = [
        Gather(net, "batch", y, d, lambda b, i=i: xs.at[z, 0, b, pl.ds(i * 32, 32)])
        for i, d in enumerate((1, -1))
    ]
    b1 = [
        Gather(net, "tensor", z, d, lambda b, i=i: xs.at[b, 1, y, pl.ds(i * 32, 32)])
        for i, d in enumerate((1, -1))
    ]
    net.used = fresh
    low, high, whole = pl.ds(0, 32), pl.ds(32, 32), pl.ds(0, 64)
    cuts = ((0, low, 1), (0, high, -1), (3, whole, 1), (1, whole, -1), (2, low, 1), (2, high, -1))
    a2 = [
        Gather(net, "tensor", z, d, lambda b, j=j, r=r: xs.at[b, 0, near(y + j), r])
        for j, r, d in cuts
    ]
    b2 = [
        Gather(net, "batch", y, d, lambda b, j=j, r=r: xs.at[near(z + j), 1, b, r])
        for j, r, d in cuts
    ]

    wait_x(0)
    b1[0].start()
    b2[0].start()
    wait_x(1)
    a1[0].start()
    a2[0].start()
    wait_x(3)
    a1[1].start()
    wait_x(2)
    b1[1].start()
    a2[1].start()
    b2[1].start()
    for piece in (b1[0], *a1, b1[1]):
        piece.relay()
    for stage, later in ((a1, a2), (b1, b2)):
        for piece in stage:
            piece.direct()
        later[2].start()
        later[3].start()
    for i in range(2):
        a1[i].last()
        a2[4 + i].start()
    b2[0].relay()
    b2[1].relay()
    for i in range(2):
        b1[i].last()
        b2[4 + i].start()
    for piece in mix_pieces:
        piece.direct()
        piece.last()

    loads[2].wait()
    loads[3].wait()
    share = acc.shape[0]

    def raise_rows(h, b, first=False, last=False):
        deep = pl.ds(pl.multiple_of(b * width, width), width)
        block = xs[b, h].reshape(RING * 64, width)
        for j in range(share):
            at = pl.ds(j * 128, 128)
            both = jnp.concatenate([wg[deep, at], wu[deep, at]], axis=1)
            part = jnp.dot(block, both, preferred_element_type=F32)
            if not first:
                part = acc[j, h] + part
            if last:
                gate, up = part[:, :128], part[:, 128:]
                hid[h, :, at] = (gate / (1.0 + jnp.exp(-gate)) * up).astype(BF16)
            else:
                acc[j, h] = part

    raise_rows(0, z, first=True)
    a2[0].relay()
    a2[1].relay()
    b2[2].relay()
    a2[2].relay()
    b2[3].relay()
    a2[3].relay()
    for piece in b2[:2]:
        piece.direct()
        piece.last()
    raise_rows(1, z, first=True)
    for piece in a2:
        piece.direct()
    a2[4].relay()
    a2[5].relay()
    raise_rows(0, near(z - 1))
    b2[4].relay()
    b2[5].relay()
    raise_rows(0, near(z + 1))
    b2[3].direct()
    b2[3].last()
    raise_rows(1, near(z + 1))
    b2[2].direct()
    b2[2].last()
    raise_rows(1, near(z - 1))
    for piece in a2:
        piece.last()
    raise_rows(0, near(z + 2), last=True)

    loads[4].wait()

    def lower_rows(h, b):
        for j in range(width // tile):
            inside = pl.ds(j * tile, tile)
            at = pl.ds(pl.multiple_of(b * width + j * tile, tile), tile)
            part = jnp.dot(hid[h], wd[:, at], preferred_element_type=F32)
            ys[b, h, :, :, inside] = part.astype(BF16).reshape(RING, 64, tile)

    order = (2, 1, 3, 0)
    sides = (1, -1, 1, -1)
    net.used = first_x
    ra1 = [
        Scatter(
            net, "tensor", z, d,
            lambda b, j=j: ys.at[b, 0, near(y + j)],
            [a_in.at[k, i] for k in range(3)],
        )
        for i, (j, d) in enumerate(zip(order, sides))
    ]
    net.used = 0
    rb1 = [
        Scatter(
            net, "batch", y, d,
            lambda b, j=j: ys.at[near(z + j), 1, b],
            [b_in.at[k, i] for k in range(3)],
        )
        for i, (j, d) in enumerate(zip(order, sides))
    ]
    net.used = token_pieces[0].n
    minor = [(kk, dc) for kk in range(2) for dc in range(2)]

    def strip(kk, dc):
        return pl.ds(kk * 32 + lax.rem(c + dc, 2) * 16, 16)

    ra2 = [
        Scatter(
            net, "batch", y, 1 - 2 * dc,
            lambda b, kk=kk, dc=dc: a_sum.at[b, strip(kk, dc)],
            [a2_in.at[k, 2 * kk + dc] for k in range(3)],
        )
        for kk, dc in minor
    ]
    rb2 = [
        Scatter(
            net, "tensor", z, 1 - 2 * dc,
            lambda b, kk=kk, dc=dc: b_sum.at[b, strip(kk, dc)],
            [b2_in.at[k, 2 * kk + dc] for k in range(3)],
        )
        for kk, dc in minor
    ]

    lower_rows(0, near(z + 2))
    for piece in ra1:
        piece.send_far()
    for piece in b2[4:]:
        piece.direct()
        piece.last()
    raise_rows(1, near(z + 2), last=True)
    lower_rows(1, near(z + 2))
    rb1[0].send_far()
    rb1[0].send_near()
    lower_rows(1, near(z + 1))
    rb1[1].send_far()
    rb1[1].send_near()
    lower_rows(0, near(z + 1))
    ra1[1].send_near()
    ra1[3].send_near()
    lower_rows(0, near(z - 1))
    ra1[0].send_near()
    ra1[2].send_near()
    lower_rows(1, near(z - 1))
    rb1[2].send_far()
    rb1[2].send_near()
    ra1[0].relay()
    ra1[1].relay()
    lower_rows(1, z)
    rb1[3].send_far()
    rb1[3].send_near()
    rb1[0].relay()
    lower_rows(0, z)
    ra1[2].relay()
    ra1[3].relay()
    rb1[1].relay()
    rb1[2].relay()
    rb1[3].relay()

    def close_sum(pieces, n, sums, me):
        sums[near(me + order[n])] = pieces[n].finish().astype(BF16)

    both = (
        (ra1, a_sum, y, (ra2[0], ra2[2]), (ra2[1], ra2[3])),
        (rb1, b_sum, z, (rb2[2], rb2[0]), (rb2[3], rb2[1])),
    )
    for stage, sums, me, plus, minus in both:
        close_sum(stage, 0, sums, me)
        for piece in (*plus, *minus):
            piece.send_far()
        close_sum(stage, 1, sums, me)
        for piece in minus:
            piece.send_near()
    for stage, sums, me, plus, minus in both:
        for piece in plus:
            piece.relay()
        close_sum(stage, 2, sums, me)
        for piece in plus:
            piece.send_near()
        for piece in minus:
            piece.relay()
    for stage, sums, me, plus, minus in both:
        close_sum(stage, 3, sums, me)

    first_back = net.take(len(across))
    backs = {step: first_back + n for n, step in enumerate(across)}
    for k, stage in ((2, rb2), (0, rb2), (1, ra2), (3, ra2)):
        for dc in range(2):
            done = stage[k // 2 * 2 + dc].finish().astype(BF16)
            if (k, dc) == (0, 0):
                rf[y, e] = done
            else:
                so[k, dc] = done
                net.start(backs[k, dc], so.at[k, dc], rf.at[y, e], over_x(k, dc))

    def source(k, dc):
        return near(x - k) * 2 + lax.rem(c + dc, 2)

    out_pieces = {
        (k, dc): Gather(
            net, "batch", y, 1 - 2 * dc, lambda b, k=k, dc=dc: rf.at[b, source(k, dc)]
        )
        for k in range(RING)
        for dc in range(2)
    }

    def start_out(k):
        for dc in range(2):
            if (k, dc) != (0, 0):
                net.arrived(backs[k, dc], rf.at[y, source(k, dc)], over_x(k, dc))
            out_pieces[k, dc].start()

    start_out(0)
    start_out(2)
    start_out(1)
    for dc in range(2):
        out_pieces[0, dc].relay()
    start_out(3)
    for k in (2, 1, 3):
        for dc in range(2):
            out_pieces[k, dc].relay()
    for piece in out_pieces.values():
        piece.direct()
    for piece in out_pieces.values():
        piece.last()

    net.drain()


SENDS, ARRIVALS = 40, 113


def local(tokens, gain, phi, w_gate, w_up, w_down):
    share = w_gate.shape[2]
    width = tokens.shape[2]
    count = tokens.shape[1]
    rows = count // RING
    slots = phi.shape[1]
    vmem = pltpu.VMEM
    scratch = [
        vmem((count, width), BF16),
        vmem((width, slots), BF16),
        vmem((D, share), BF16),
        vmem((D, share), BF16),
        vmem((share, D), BF16),
        vmem((RING, count, width), BF16),
        vmem((RING, rows, slots), F32),
        vmem((3, 4, 16, slots), F32),
        vmem((RING, 8, 128), F32),
        vmem((3, 8, 128), F32),
        vmem((RING, 2, 128), F32),
        vmem((RING, RING, 2, 128), F32),
        vmem((RING, rows, 128), BF16),
        vmem((RING, RING, rows, 128), BF16),
        vmem((128, RING * count), BF16),
        vmem((8, 16, width), BF16),
        vmem((RING, 2, RING, 64, width), BF16),
        vmem((share // 128, 2, 256, 256), F32),
        vmem((2, 256, share), BF16),
        vmem((RING, 2, RING, 64, width), BF16),
        vmem((3, 4, 64, width), BF16),
        vmem((RING, 64, width), BF16),
        vmem((3, 4, 16, width), BF16),
        vmem((3, 4, 64, width), BF16),
        vmem((RING, 64, width), BF16),
        vmem((3, 4, 16, width), BF16),
        vmem((4, 2, 16, width), BF16),
        pltpu.SemaphoreType.DMA((5,)),
        pltpu.SemaphoreType.DMA((SENDS,)),
        pltpu.SemaphoreType.DMA((ARRIVALS,)),
    ]
    anywhere = pl.BlockSpec(memory_space=pltpu.HBM)
    inside = pl.BlockSpec(memory_space=vmem)
    mix, slot_rows = pl.pallas_call(
        kernel,
        out_shape=[
            jax.ShapeDtypeStruct((RING, rows, slots), BF16),
            jax.ShapeDtypeStruct((RING, 8, 16, width), BF16),
        ],
        in_specs=[anywhere, inside, anywhere, anywhere, anywhere, anywhere],
        out_specs=[inside, inside],
        scratch_shapes=scratch,
        compiler_params=pltpu.CompilerParams(
            collective_id=0, has_side_effects=True, vmem_limit_bytes=48 << 20
        ),
        name="soft_moe",
    )(keep(tokens[0]), keep(gain.reshape(-1, 128)), keep(phi), w_gate[0], w_up[0], w_down[0])
    out = jnp.dot(
        mix.reshape(count, slots), slot_rows.reshape(slots, width), preferred_element_type=F32
    )
    return out.astype(BF16)[None]


def solution(mesh):
    placed = (
        P("expert", "batch", "tensor"),
        P("tensor"),
        P("tensor", None),
        P("expert", None, ("batch", "tensor")),
        P("expert", None, ("batch", "tensor")),
        P("expert", ("batch", "tensor"), None),
    )
    return jax.shard_map(
        local, mesh=mesh, in_specs=placed, out_specs=P("expert", "batch", "tensor"), check_vma=False
    )
```

```python
import jax
import jax.numpy as jnp
from jax import lax
from jax.experimental import pallas as pl
from jax.experimental.pallas import tpu as pltpu
from jax.sharding import PartitionSpec as P


D = 4096
RING = 4
BF16 = jnp.bfloat16
F32 = jnp.float32


def keep(v):
    return pltpu.with_memory_space_constraint(v, pltpu.HBM)


def near(v):
    return lax.rem(v + 2 * RING, RING)


class Net:
    def __init__(self, send_sems, recv_sems):
        self.send_sems, self.recv_sems = send_sems, recv_sems
        self.used, self.count, self.sent = 0, 0, {}

    def take(self, count):
        first = self.used
        self.used += count
        return first

    def copy(self, n, src, dst, target):
        return pltpu.make_async_remote_copy(
            src_ref=src,
            dst_ref=dst,
            send_sem=self.send_sems.at[self.count % SENDS],
            recv_sem=self.recv_sems.at[n],
            device_id=target,
            device_id_type=pl.DeviceIdType.MESH,
        )

    def start(self, n, src, dst, target):
        slot = self.count % SENDS
        if slot in self.sent:
            self.sent[slot].wait_send()
        one = self.copy(n, src, dst, target)
        one.start()
        self.sent[slot] = one
        self.count += 1

    def arrived(self, n, dst, target):
        self.copy(n, dst, dst, target).wait_recv()

    def drain(self):
        for one in self.sent.values():
            one.wait_send()


class Gather:
    def __init__(self, net, axis, me, d, ref):
        self.net, self.axis, self.me, self.d, self.ref = net, axis, me, d, ref
        self.n = net.take(3)

    def to(self, d):
        return {self.axis: near(self.me + d)}

    def start(self):
        mine = self.ref(self.me)
        self.net.start(self.n, mine, mine, self.to(self.d))
        self.net.start(self.n + 1, mine, mine, self.to(-self.d))

    def relay(self):
        block = self.ref(near(self.me - self.d))
        self.net.arrived(self.n, block, self.to(self.d))
        self.net.start(self.n + 2, block, block, self.to(self.d))

    def direct(self):
        self.net.arrived(self.n + 1, self.ref(near(self.me + self.d)), self.to(self.d))

    def last(self):
        self.net.arrived(self.n + 2, self.ref(near(self.me + 2)), self.to(self.d))


class Scatter:
    def __init__(self, net, axis, me, d, part, buffers):
        self.net, self.axis, self.me, self.d, self.part = net, axis, me, d, part
        self.passing, self.direct_in, self.joined = buffers
        self.n = net.take(3)

    def to(self, d):
        return {self.axis: near(self.me + d)}

    def send_far(self):
        self.net.start(self.n, self.part(near(self.me + 2)), self.passing, self.to(self.d))

    def send_near(self):
        self.net.start(self.n + 1, self.part(near(self.me - self.d)), self.direct_in, self.to(-self.d))

    def relay(self):
        self.net.arrived(self.n, self.passing, self.to(self.d))
        term = self.part(near(self.me + self.d))
        total = term[...].astype(F32) + self.passing[...].astype(F32)
        term[...] = total.astype(term.dtype)
        self.net.start(self.n + 2, term, self.joined, self.to(self.d))

    def finish(self):
        self.net.arrived(self.n + 1, self.direct_in, self.to(self.d))
        self.net.arrived(self.n + 2, self.joined, self.to(self.d))
        mine = self.part(self.me)[...].astype(F32)
        return mine + self.direct_in[...].astype(F32) + self.joined[...].astype(F32)


def kernel(
    tok_in, gain, phi_in, wg_in, wu_in, wd_in, cb, rf,
    tok, phi, wg, wu, wd, tg,
    lp, l_in, sq_out, sq_in, sx, st, qo, qg, qt,
    si, xs, acc, hid, ys,
    a_in, a_sum, a2_in, b_in, b_sum, b2_in, so,
    load_sems, send_sems, recv_sems,
):
    y = lax.axis_index("batch")
    e = lax.axis_index("expert")
    z = lax.axis_index("tensor")
    x, c = e // 2, lax.rem(e, 2)

    loads = [
        pltpu.make_async_copy(src, dst, load_sems.at[i])
        for i, (src, dst) in enumerate(
            ((tok_in, tok), (phi_in, phi), (wg_in, wg), (wu_in, wu), (wd_in, wd))
        )
    ]
    loads[0].start()
    loads[1].start()

    barrier = pltpu.get_barrier_semaphore()
    plane = [(dy, dz) for dy in range(RING) for dz in range(RING) if (dy, dz) != (0, 0)]
    across = [(dx, dc) for dx in (0, 1, 3, 2) for dc in range(2) if (dx, dc) != (0, 0)]

    def in_plane(dy, dz):
        return {"batch": near(y + dy), "tensor": near(z + dz)}

    def over_x(dx, dc):
        return {"expert": near(x + dx) * 2 + lax.rem(c + dc, 2)}

    peers = [in_plane(*step) for step in plane] + [over_x(*step) for step in across]
    for peer in peers:
        pl.semaphore_signal(
            barrier, inc=1, device_id=peer, device_id_type=pl.DeviceIdType.MESH
        )

    net = Net(send_sems, recv_sems)

    rows = lp.shape[1]
    width = tok.shape[1]
    wide = jnp.concatenate([gain[k : k + 1, :] for k in range(width // 128)], axis=1)
    loads[0].wait()
    tokens_f = tok[...].astype(F32)
    scaled = (tokens_f * wide.astype(F32)).astype(BF16)
    tg[y] = scaled
    loads[1].wait()
    part = jnp.dot(scaled, phi[...], preferred_element_type=F32)
    lp[...] = part.reshape(lp.shape)
    for one in loads[2:]:
        one.start()

    pl.semaphore_wait(barrier, len(peers))

    half = rows // 2
    logit_pieces = [
        Scatter(
            net, "tensor", z, d,
            lambda b, i=i: lp.at[b, pl.ds(i * 16, 16)],
            [l_in.at[k, i] for k in range(3)],
        )
        for i, d in enumerate((1, -1, 1, -1))
    ]
    token_pieces = [
        Gather(net, "batch", y, d, lambda b, i=i: tg.at[b, :, pl.ds(i * 256, 256)])
        for i, d in enumerate((1, -1, 1, -1))
    ]
    for piece in logit_pieces:
        piece.send_far()
    for piece in logit_pieces:
        piece.send_near()
    token_pieces[0].start()
    token_pieces[1].start()

    squares = jnp.sum(tokens_f * tokens_f, axis=1, keepdims=True)
    diagonal = lax.broadcasted_iota(jnp.int32, (rows, 128), 0) == lax.broadcasted_iota(
        jnp.int32, (rows, 128), 1
    )
    for b in range(RING):
        column = squares[b * rows : (b + 1) * rows]
        line = jnp.sum(jnp.where(diagonal, column, 0.0), axis=0, keepdims=True)
        sq_out[b] = jnp.broadcast_to(line, (8, 128))
    first_sq = net.take(3)
    for k in range(3):
        to = near(z + k + 1)
        net.start(first_sq + k, sq_out.at[to], sq_in.at[k], {"tensor": to})
    for piece in logit_pieces:
        piece.relay()
    token_pieces[2].start()
    for k in range(3):
        net.arrived(first_sq + k, sq_in.at[k], {"tensor": near(z + k + 1)})
    sq = sq_out[z] + sq_in[0] + sq_in[1] + sq_in[2]
    sq_column = jnp.sum(jnp.where(diagonal, sq[0:1, :], 0.0), axis=1, keepdims=True)
    inv_rms = lax.rsqrt(sq_column / D + 1e-06)
    logits = jnp.concatenate([piece.finish() for piece in logit_pieces], axis=0) * inv_rms

    lane = lax.broadcasted_iota(jnp.int32, (rows, 128), 1)
    quarters = []
    for q in range(RING):
        made = jnp.zeros((rows, 128), F32)
        for n in range(8):
            source = logits[:, n // 2 * 128 : n // 2 * 128 + 128]
            shift = (n * 16 - n % 2 * 64 - q * 16) % 128
            moved = pltpu.roll(source, shift, 1) if shift else source
            made = jnp.where((lane >= n * 16) & (lane < n * 16 + 16), moved, made)
        quarters.append(made)
    logits = jnp.concatenate(quarters, axis=1)

    local_max = jnp.max(logits, axis=0, keepdims=True)
    raised = jnp.exp(logits - local_max)
    local_total = jnp.sum(raised, axis=0, keepdims=True)
    for k in range(RING):
        sx[k, 0:1, :] = local_max[:, k * 128 : (k + 1) * 128]
        sx[k, 1:2, :] = local_total[:, k * 128 : (k + 1) * 128]
    st[y, z] = sx[y]
    factor = (raised * inv_rms).astype(BF16)
    for k in range(RING):
        qo[k] = factor[:, k * 128 : (k + 1) * 128]
    qg[z, y] = qo[y]
    first_q = net.take(3)
    for k in (1, 0, 2):
        to = near(y + k + 1)
        net.start(first_q + k, qo.at[to], qg.at[z, y], {"batch": to})
    first_qz = net.take(12)

    def spread(k):
        block = qg.at[z, near(y - k)]
        for n in (0, 2, 1):
            net.start(first_qz + 3 * k + n, block, block, {"tensor": near(z + n + 1)})

    spread(0)
    first_st = net.take(len(plane))
    for k, step in enumerate(plane):
        net.start(first_st + k, sx.at[near(y + step[0])], st.at[y, z], in_plane(*step))
    token_pieces[3].start()
    token_pieces[0].relay()
    token_pieces[1].relay()

    row_max = jnp.max(logits, axis=1, keepdims=True)
    row_raised = jnp.exp(logits - row_max)
    cb[z] = (row_raised / jnp.sum(row_raised, axis=1, keepdims=True)).astype(BF16)
    mix_pieces = [
        Gather(net, "tensor", z, d, lambda b, i=i: cb.at[b, pl.ds(i * half, half)])
        for i, d in enumerate((1, -1))
    ]
    for piece in mix_pieces:
        piece.start()
    for k in (1, 3, 2):
        net.arrived(first_q + k - 1, qg.at[z, near(y - k)], {"batch": near(y + k)})
        spread(k)
        if k == 3:
            token_pieces[2].relay()
    token_pieces[3].relay()
    for k, (dy, dz) in enumerate(plane):
        net.arrived(first_st + k, st.at[near(y - dy), near(z - dz)], in_plane(dy, dz))
    maxima = st[:, :, 0:1, :]
    totals = st[:, :, 1:2, :]
    top = jnp.max(jnp.max(maxima, axis=1, keepdims=True), axis=0, keepdims=True)
    weights = jnp.exp(maxima - top)
    total = jnp.sum(jnp.sum(totals * weights, axis=1, keepdims=True), axis=0, keepdims=True)
    weights = weights / total
    for piece in mix_pieces:
        piece.relay()
    for k in (0, 1, 3, 2):
        for n in range(3):
            net.arrived(
                first_qz + 3 * k + n,
                qg.at[near(z - n - 1), near(y - k)],
                {"tensor": near(z + n + 1)},
            )
    for b in range(RING):
        scaled_q = jnp.concatenate(
            [qg[k, b].astype(F32) * weights[b, k] for k in range(RING)], axis=0
        )
        qt[:, b * RING * rows : (b + 1) * RING * rows] = scaled_q.T.astype(BF16)
    tile = 256

    def place(k, core, part):
        inside = pl.ds(k // 2 * 32 + core * 16, 16)
        return xs.at[z, (k + 1) % 2, y, inside, pl.ds(part * 2 * tile, 2 * tile)]

    first_x = net.take(2 * len(across))
    for part in range(2):
        for piece in token_pieces[2 * part : 2 * part + 2]:
            piece.direct()
            piece.last()
        for j in (2 * part, 2 * part + 1):
            at = pl.ds(j * tile, tile)
            made = jnp.dot(
                qt[...], tg[:, :, at].reshape(qt.shape[1], tile), preferred_element_type=F32
            )
            si[:, :, at] = made.astype(BF16).reshape(8, 16, tile)
        own = pl.ds(part * 2 * tile, 2 * tile)
        for n, (dx, dc) in enumerate(across):
            target = over_x(dx, dc)
            net.start(
                first_x + 2 * n + part,
                si.at[target["expert"], :, own],
                place((RING - dx) % RING, c, part),
                target,
            )
        place(0, c, part)[...] = si[e, :, own]

    def wait_x(k):
        for n, (dx, dc) in enumerate(across):
            if (RING - dx) % RING == k:
                for part in range(2):
                    net.arrived(
                        first_x + 2 * n + part,
                        place(k, lax.rem(c + dc, 2), part),
                        over_x(dx, dc),
                    )

    fresh, net.used = net.used, 0
    a1 = [
        Gather(net, "batch", y, d, lambda b, i=i: xs.at[z, 0, b, pl.ds(i * 32, 32)])
        for i, d in enumerate((1, -1))
    ]
    b1 = [
        Gather(net, "tensor", z, d, lambda b, i=i: xs.at[b, 1, y, pl.ds(i * 32, 32)])
        for i, d in enumerate((1, -1))
    ]
    net.used = fresh
    low, high, whole = pl.ds(0, 32), pl.ds(32, 32), pl.ds(0, 64)
    cuts = ((0, low, 1), (0, high, -1), (3, whole, 1), (1, whole, -1), (2, low, 1), (2, high, -1))
    a2 = [
        Gather(net, "tensor", z, d, lambda b, j=j, r=r: xs.at[b, 0, near(y + j), r])
        for j, r, d in cuts
    ]
    b2 = [
        Gather(net, "batch", y, d, lambda b, j=j, r=r: xs.at[near(z + j), 1, b, r])
        for j, r, d in cuts
    ]

    wait_x(0)
    b1[0].start()
    b2[0].start()
    wait_x(1)
    a1[0].start()
    a2[0].start()
    wait_x(3)
    a1[1].start()
    wait_x(2)
    b1[1].start()
    a2[1].start()
    b2[1].start()
    for piece in (b1[0], *a1, b1[1]):
        piece.relay()
    for stage, later in ((a1, a2), (b1, b2)):
        for piece in stage:
            piece.direct()
        later[2].start()
        later[3].start()
    for i in range(2):
        a1[i].last()
        a2[4 + i].start()
    b2[0].relay()
    b2[1].relay()
    for i in range(2):
        b1[i].last()
        b2[4 + i].start()
    for piece in mix_pieces:
        piece.direct()
        piece.last()

    loads[2].wait()
    loads[3].wait()
    share = acc.shape[0]

    def raise_rows(h, b, first=False, last=False):
        deep = pl.ds(pl.multiple_of(b * width, width), width)
        block = xs[b, h].reshape(RING * 64, width)
        for j in range(share):
            at = pl.ds(j * 128, 128)
            both = jnp.concatenate([wg[deep, at], wu[deep, at]], axis=1)
            part = jnp.dot(block, both, preferred_element_type=F32)
            if not first:
                part = acc[j, h] + part
            if last:
                gate, up = part[:, :128], part[:, 128:]
                hid[h, :, at] = (gate / (1.0 + jnp.exp(-gate)) * up).astype(BF16)
            else:
                acc[j, h] = part

    raise_rows(0, z, first=True)
    a2[0].relay()
    a2[1].relay()
    b2[2].relay()
    a2[2].relay()
    b2[3].relay()
    a2[3].relay()
    for piece in b2[:2]:
        piece.direct()
        piece.last()
    raise_rows(1, z, first=True)
    for piece in a2:
        piece.direct()
    a2[4].relay()
    a2[5].relay()
    raise_rows(0, near(z - 1))
    b2[4].relay()
    b2[5].relay()
    raise_rows(0, near(z + 1))
    b2[3].direct()
    b2[3].last()
    raise_rows(1, near(z + 1))
    b2[2].direct()
    b2[2].last()
    raise_rows(1, near(z - 1))
    for piece in a2:
        piece.last()
    raise_rows(0, near(z + 2), last=True)

    loads[4].wait()

    def lower_rows(h, b):
        for j in range(width // tile):
            inside = pl.ds(j * tile, tile)
            at = pl.ds(pl.multiple_of(b * width + j * tile, tile), tile)
            part = jnp.dot(hid[h], wd[:, at], preferred_element_type=F32)
            ys[b, h, :, :, inside] = part.astype(BF16).reshape(RING, 64, tile)

    order = (2, 1, 3, 0)
    sides = (1, -1, 1, -1)
    net.used = first_x
    ra1 = [
        Scatter(
            net, "tensor", z, d,
            lambda b, j=j: ys.at[b, 0, near(y + j)],
            [a_in.at[k, i] for k in range(3)],
        )
        for i, (j, d) in enumerate(zip(order, sides))
    ]
    net.used = 0
    rb1 = [
        Scatter(
            net, "batch", y, d,
            lambda b, j=j: ys.at[near(z + j), 1, b],
            [b_in.at[k, i] for k in range(3)],
        )
        for i, (j, d) in enumerate(zip(order, sides))
    ]
    net.used = token_pieces[0].n
    minor = [(kk, dc) for kk in range(2) for dc in range(2)]

    def strip(kk, dc):
        return pl.ds(kk * 32 + lax.rem(c + dc, 2) * 16, 16)

    ra2 = [
        Scatter(
            net, "batch", y, 1 - 2 * dc,
            lambda b, kk=kk, dc=dc: a_sum.at[b, strip(kk, dc)],
            [a2_in.at[k, 2 * kk + dc] for k in range(3)],
        )
        for kk, dc in minor
    ]
    rb2 = [
        Scatter(
            net, "tensor", z, 1 - 2 * dc,
            lambda b, kk=kk, dc=dc: b_sum.at[b, strip(kk, dc)],
            [b2_in.at[k, 2 * kk + dc] for k in range(3)],
        )
        for kk, dc in minor
    ]

    lower_rows(0, near(z + 2))
    for piece in ra1:
        piece.send_far()
    for piece in b2[4:]:
        piece.direct()
        piece.last()
    raise_rows(1, near(z + 2), last=True)
    lower_rows(1, near(z + 2))
    rb1[0].send_far()
    rb1[0].send_near()
    lower_rows(1, near(z + 1))
    rb1[1].send_far()
    rb1[1].send_near()
    lower_rows(0, near(z + 1))
    ra1[1].send_near()
    ra1[3].send_near()
    lower_rows(0, near(z - 1))
    ra1[0].send_near()
    ra1[2].send_near()
    lower_rows(1, near(z - 1))
    rb1[2].send_far()
    rb1[2].send_near()
    ra1[0].relay()
    ra1[1].relay()
    lower_rows(1, z)
    rb1[0].relay()
    rb1[3].send_far()
    rb1[3].send_near()
    lower_rows(0, z)
    ra1[2].relay()
    ra1[3].relay()
    rb1[1].relay()
    rb1[2].relay()
    rb1[3].relay()

    def close_sum(pieces, n, sums, me):
        sums[near(me + order[n])] = pieces[n].finish().astype(BF16)

    both = (
        (ra1, a_sum, y, (ra2[0], ra2[2]), (ra2[1], ra2[3])),
        (rb1, b_sum, z, (rb2[2], rb2[0]), (rb2[3], rb2[1])),
    )
    for stage, sums, me, plus, minus in both:
        close_sum(stage, 0, sums, me)
        for piece in (*plus, *minus):
            piece.send_far()
        close_sum(stage, 1, sums, me)
        for piece in minus:
            piece.send_near()
    for stage, sums, me, plus, minus in both:
        for piece in plus:
            piece.relay()
        close_sum(stage, 2, sums, me)
        for piece in plus:
            piece.send_near()
        for piece in minus:
            piece.relay()
    for stage, sums, me, plus, minus in both:
        close_sum(stage, 3, sums, me)

    first_back = net.take(len(across))
    backs = {step: first_back + n for n, step in enumerate(across)}
    for k, stage in ((2, rb2), (0, rb2), (1, ra2), (3, ra2)):
        for dc in range(2):
            done = stage[k // 2 * 2 + dc].finish().astype(BF16)
            if (k, dc) == (0, 0):
                rf[y, e] = done
            else:
                so[k, dc] = done
                net.start(backs[k, dc], so.at[k, dc], rf.at[y, e], over_x(k, dc))

    def source(k, dc):
        return near(x - k) * 2 + lax.rem(c + dc, 2)

    out_pieces = {
        (k, dc): Gather(
            net, "batch", y, 1 - 2 * dc, lambda b, k=k, dc=dc: rf.at[b, source(k, dc)]
        )
        for k in range(RING)
        for dc in range(2)
    }

    def start_out(k):
        for dc in range(2):
            if (k, dc) != (0, 0):
                net.arrived(backs[k, dc], rf.at[y, source(k, dc)], over_x(k, dc))
            out_pieces[k, dc].start()

    start_out(0)
    start_out(2)
    start_out(1)
    for dc in range(2):
        out_pieces[0, dc].relay()
    start_out(3)
    for k in (2, 1, 3):
        for dc in range(2):
            out_pieces[k, dc].relay()
    for piece in out_pieces.values():
        piece.direct()
    for piece in out_pieces.values():
        piece.last()

    net.drain()


SENDS, ARRIVALS = 40, 113


def local(tokens, gain, phi, w_gate, w_up, w_down):
    share = w_gate.shape[2]
    width = tokens.shape[2]
    count = tokens.shape[1]
    rows = count // RING
    slots = phi.shape[1]
    vmem = pltpu.VMEM
    scratch = [
        vmem((count, width), BF16),
        vmem((width, slots), BF16),
        vmem((D, share), BF16),
        vmem((D, share), BF16),
        vmem((share, D), BF16),
        vmem((RING, count, width), BF16),
        vmem((RING, rows, slots), F32),
        vmem((3, 4, 16, slots), F32),
        vmem((RING, 8, 128), F32),
        vmem((3, 8, 128), F32),
        vmem((RING, 2, 128), F32),
        vmem((RING, RING, 2, 128), F32),
        vmem((RING, rows, 128), BF16),
        vmem((RING, RING, rows, 128), BF16),
        vmem((128, RING * count), BF16),
        vmem((8, 16, width), BF16),
        vmem((RING, 2, RING, 64, width), BF16),
        vmem((share // 128, 2, 256, 256), F32),
        vmem((2, 256, share), BF16),
        vmem((RING, 2, RING, 64, width), BF16),
        vmem((3, 4, 64, width), BF16),
        vmem((RING, 64, width), BF16),
        vmem((3, 4, 16, width), BF16),
        vmem((3, 4, 64, width), BF16),
        vmem((RING, 64, width), BF16),
        vmem((3, 4, 16, width), BF16),
        vmem((4, 2, 16, width), BF16),
        pltpu.SemaphoreType.DMA((5,)),
        pltpu.SemaphoreType.DMA((SENDS,)),
        pltpu.SemaphoreType.DMA((ARRIVALS,)),
    ]
    anywhere = pl.BlockSpec(memory_space=pltpu.HBM)
    inside = pl.BlockSpec(memory_space=vmem)
    mix, slot_rows = pl.pallas_call(
        kernel,
        out_shape=[
            jax.ShapeDtypeStruct((RING, rows, slots), BF16),
            jax.ShapeDtypeStruct((RING, 8, 16, width), BF16),
        ],
        in_specs=[anywhere, inside, anywhere, anywhere, anywhere, anywhere],
        out_specs=[inside, inside],
        scratch_shapes=scratch,
        compiler_params=pltpu.CompilerParams(
            collective_id=0, has_side_effects=True, vmem_limit_bytes=48 << 20
        ),
        name="soft_moe",
    )(keep(tokens[0]), keep(gain.reshape(-1, 128)), keep(phi), w_gate[0], w_up[0], w_down[0])
    out = jnp.dot(
        mix.reshape(count, slots), slot_rows.reshape(slots, width), preferred_element_type=F32
    )
    return out.astype(BF16)[None]


def solution(mesh):
    placed = (
        P("expert", "batch", "tensor"),
        P("tensor"),
        P("tensor", None),
        P("expert", None, ("batch", "tensor")),
        P("expert", None, ("batch", "tensor")),
        P("expert", ("batch", "tensor"), None),
    )
    return jax.shard_map(
        local, mesh=mesh, in_specs=placed, out_specs=P("expert", "batch", "tensor"), check_vma=False
    )
```
